32 devices in a mesh: gx: 4 (over z), gy: 4 (over y, x), gz: 2 (over core).
Axes of the slice: x: 2, y: 2, z: 4, core: 2. Of those that a mesh axis runs over, the one named last changes fastest.
Arguments:
- volume: float32 [32, 256, 4096], P('gz', 'gy', 'gx'), may hold values from -24 to 24
Outputs:
- level_one: float32 [16, 128, 2048], P('gz', 'gy', 'gx')
- level_two: float32 [8, 64, 1024], P('gz', 'gy', 'gx')
- level_three: float32 [4, 32, 512], P('gz', 'gy', 'gx')
The draws below stay inside these ranges and needn't reach their ends.
All inputs are finite; a program needn't handle non-finite values.
Results may differ from the reference program's by a relative error of at most 0.00002.
Values sent between devices are 32-bit elements; how exact they have to be, the bound alone decides.
A program may use at most 64 MiB of HBM per device.

```python
import jax
import jax.numpy as jnp
from jax import lax

NX = 4096
NY = 256
NZ = 32


def shard_levels(stream_key, shape, split, smallest, largest):
    level = 1.0
    for dim, shards_of in split:
        draws = jax.random.uniform(jax.random.fold_in(jax.random.fold_in(stream_key, 6), dim), (shards_of,), jnp.float32, smallest / len(split), largest / len(split))
        level = level * jnp.repeat(jnp.exp(draws), shape[dim] // shards_of).reshape((-1,) + (1,) * (len(shape) - 1 - dim))
    return level


def gaussian(rng, dims, deviation, most, cuts=(), kind=jnp.bfloat16):
    result = deviation * jax.random.normal(rng, dims, jnp.float32)
    if cuts:
        result = result * shard_levels(rng, dims, cuts, -0.22, 0.18)
    return jnp.clip(result, -most, most).astype(kind)


def setup_inputs(seed: int = 0) -> dict:
    streams_of = jax.random.split(jax.random.key(seed), 2)
    return {
        "volume": gaussian(streams_of[0], (NZ, NY, NX), 4.0, 24.0, ((0, 2), (1, 4), (2, 4)), jnp.float32),
    }


taps = (0.0625, 0.25, 0.375, 0.25, 0.0625)


def reduce_padded(padded, dim, count):
    total = None
    for k in range(5):
        piece = lax.slice_in_dim(padded, k, k + 2 * count - 1, 2, dim)
        term = taps[k] * piece
        total = term if total is None else total + term
    return total


def reduce_axis(field, dim):
    widths = [(0, 0), (0, 0), (0, 0)]
    widths[dim] = (2, 2)
    padded = jnp.pad(field, widths)
    return reduce_padded(padded, dim, field.shape[dim] // 2)


def level_down(field):
    return reduce_axis(reduce_axis(reduce_axis(field, 0), 1), 2)


def reference(volume):
    level_one = level_down(volume)
    level_two = level_down(level_one)
    level_three = level_down(level_two)
    return level_one, level_two, level_three
```

```python
import functools
import itertools

import jax
import jax.numpy as jnp
import numpy as np
from jax import lax
from jax.experimental import pallas as pl
from jax.experimental.pallas import tpu as pltpu
from jax.sharding import PartitionSpec as P

LANES = 128
MESH = pl.DeviceIdType.MESH
AXES = ("gz", "gy", "gx")
TAPS = {-2: 1, -1: 4, 0: 6, 1: 4, 2: 1}
HI = (1, 2, 2)
WIDE = (256, 128, 128)
f32, bf16 = jnp.float32, jnp.bfloat16


def chain(n, lo, hi):
    prev = {i: {i: 1} for i in range(n)}
    levels = []
    for lev in range(3):
        n //= 2
        cur = {}
        for o in range(-1 if lo else 0, n + (HI[lev] if hi else 0)):
            col = {}
            for j, w in TAPS.items():
                for k, v in prev.get(2 * o + j, {}).items():
                    col[k] = col.get(k, 0) + w * v
            cur[o] = col
        levels.append(cur)
        prev = cur
    return levels


def split2(x):
    hi = x.astype(bf16)
    return hi, (x - hi.astype(f32)).astype(bf16)


def blocks_of(lev, nt):
    per = WIDE[lev] * (2 << lev) // LANES
    return [(b, list(range(max(per * b - 1, 0), min(per * (b + 1) + 1, nt))))
            for b in range(nt // per)]


class Rows:
    def __init__(self, m, tiles):
        self.own, at = [], 0
        for lev in range(3):
            self.own.append(at)
            at += HI[lev] * tiles[lev] * m[lev]
        self.n_own = -(-at // 8) * 8
        self.hi, at = [], self.n_own
        for lev in range(3):
            self.hi.append(at)
            at += HI[lev] * tiles[lev] * HI[lev]
        self.n_hi = -(-(at - self.n_own) // 8) * 8
        self.lo, at = [], self.n_own + self.n_hi
        for lev in range(3):
            self.lo.append(at)
            at += HI[lev] * tiles[lev]
        self.n_lo = -(-(at - self.n_own - self.n_hi) // 8) * 8
        self.total = self.n_own + self.n_hi + self.n_lo


def conv(load):
    return (load(-2) + load(2)) + 4.0 * (load(-1) + load(1)) + 6.0 * load(0)


def partial_conv(load, o, lo, hi):
    have = [j for j in TAPS if lo <= 2 * o + j < hi]
    if len(have) == 5:
        return conv(lambda j: load(2 * o + j))
    total = None
    for j in have:
        term = load(2 * o + j)
        if TAPS[j] != 1:
            term = float(TAPS[j]) * term
        total = term if total is None else total + term
    return total


def kernel(sizes, dims, vol, out1, out2, out3,
           v, Z, A2Z, A3Z, EA1, EA2, EG2, EG3, YG, YX, LX1, LX2, LX3,
           W1, W2, W3, WG, DS, YS, YR, XS, XR, ZS, ZR,
           load_sem, send_sem, recv_sem):
    nz, ny, nt = dims
    m = [nz >> 1, nz >> 2, nz >> 3]
    rw = [ny >> 1, ny >> 2, ny >> 3]
    ext = [m[l] + 1 + HI[l] for l in range(3)]
    tiles = [nt >> 1, nt >> 2, nt >> 3]
    ZP, P2, P3 = ny + 3, rw[0] + 3, rw[1] + 3
    E1P, E2P = 2 * ext[1] + 3, 2 * ext[2] + 3
    rowmap = Rows(m, tiles)
    outs = (out1, out2, out3)

    idx = {a: lax.axis_index(a) for a in AXES}
    has, near = {}, {}
    for a in AXES:
        has[a, -1], has[a, 1] = idx[a] > 0, idx[a] < sizes[a] - 1
        near[a, -1] = jnp.maximum(idx[a] - 1, 0)
        near[a, 1] = jnp.minimum(idx[a] + 1, sizes[a] - 1)

    def exists(steps):
        found = None
        for a, d in steps.items():
            found = has[a, d] if found is None else jnp.logical_and(found, has[a, d])
        return found

    def device(steps):
        return {a: near[a, d] for a, d in steps.items()}

    def flag(a, d):
        return jnp.where(has[a, d], 1.0, 0.0).astype(f32)

    fz_lo, fz_hi = flag("gz", -1), flag("gz", 1)
    fy_lo, fy_hi = flag("gy", -1), flag("gy", 1)
    fx_lo, fx_hi = flag("gx", -1), flag("gx", 1)

    low, high = 8, ny - 16
    loads = []
    for i, (r0, rn) in enumerate(((0, low), (high, 16), (low, high - low))):
        c = pltpu.make_async_copy(
            vol.at[:, pl.ds(r0, rn), :], v.at[:, pl.ds(r0, rn), :], load_sem.at[i])
        c.start()
        loads.append(c)

    YR[...] = jnp.zeros(YR.shape, f32)
    XR[...] = jnp.zeros(XR.shape, f32)
    ZR[...] = jnp.zeros(ZR.shape, f32)
    peers = []
    for dz, dy, dx in itertools.product((0, -1, 1), repeat=3):
        p = {a: d for a, d in zip(AXES, (dz, dy, dx)) if d}
        if p:
            peers.append(p)
    barrier = pltpu.get_barrier_semaphore()
    for p in peers:
        @pl.when(exists(p))
        def _():
            pl.semaphore_signal(barrier, inc=1, device_id=device(p), device_id_type=MESH)

    zero = jnp.zeros((8, LANES), f32)

    def clear(ref, at, n):
        ref[at:at + n] = jnp.zeros((n, LANES), f32)

    clear(Z, 0, 2)

    @pl.loop(1, nt * ext[0])
    def _(i):
        Z[pl.ds(i * ZP - 1, 3)] = jnp.zeros((3, LANES), f32)
    clear(Z, nt * ext[0] * ZP - 1, 1)
    for s in range(ext[1]):
        clear(A2Z, s * P2, 1)
    for s in range(ext[2]):
        clear(A3Z, s * P3, 1)
    EA1[...] = jnp.zeros(EA1.shape, f32)
    EA2[...] = jnp.zeros(EA2.shape, f32)
    YG[...] = jnp.zeros(YG.shape, f32)

    row8 = lax.broadcasted_iota(jnp.int32, (8, LANES), 0)
    lane = lax.broadcasted_iota(jnp.int32, (8, LANES), 1)
    nx = nt * LANES
    full, no_lo, no_hi = chain(nx, True, True), chain(nx, False, True), chain(nx, True, False)

    def spots(entries):
        x = jnp.zeros((8, LANES), f32)
        for r, c, val in entries:
            x = jnp.where(jnp.logical_and(row8 == r, lane == c), float(val), x)
        return x

    def fixes(lev, other):
        found = {}
        for c in range(nx >> (lev + 1)):
            for k, val in full[lev][c].items():
                gone = val - other[lev].get(c, {}).get(k, 0)
                if gone:
                    found[k, c] = gone
        return found

    for lev, W in ((0, W1), (1, W2), (2, W3)):
        step = 2 << lev
        mid = (nx >> (lev + 1)) // 2
        tap = {k - step * mid: w for k, w in full[lev][mid].items()}
        reach = max(tap)
        scale = 2.0 ** (-12 * (lev + 1))
        signed = jnp.where(lane < LANES // 2, lane, lane - LANES)
        delta = row8 - step * signed
        dist = jnp.abs(delta)
        base = jnp.zeros((8, LANES), f32)
        for d in range(reach + 1):
            base = jnp.where(dist == d, tap[d] * scale, base)
        lo_fix, hi_fix = fixes(lev, no_lo), fixes(lev, no_hi)
        for b, lts in blocks_of(lev, nt):
            for part in range(WIDE[lev] // LANES):
                c0 = WIDE[lev] * b + LANES * part
                for kk in range(0, len(lts) * LANES, 16):
                    pieces = []
                    for k8 in (kk, kk + 8):
                        k = lts[0] * LANES + k8
                        first = -((-(k - reach)) // step) - c0
                        last = (k + 7 + reach) // step - c0
                        if last < 0 or first >= LANES:
                            pieces.append(zero)
                            continue
                        x = pltpu.roll(base, (k // step - c0) % LANES, 1)
                        if first < 0:
                            x = jnp.where(lane <= last, x, 0.0)
                        elif last >= LANES:
                            x = jnp.where(lane >= first, x, 0.0)
                        for fix, fl in ((lo_fix, fx_lo), (hi_fix, fx_hi)):
                            here = [(r - k, c - c0, val * scale) for (r, c), val in fix.items()
                                    if k <= r < k + 8 and c0 <= c < c0 + LANES]
                            if here:
                                x = x - (1.0 - fl) * spots(here)
                        pieces.append(x)
                    w = jnp.concatenate(pieces, axis=0)
                    hi = w.astype(bf16)
                    cols = slice(part * LANES, (part + 1) * LANES)
                    if lev < 2:
                        W[b, kk:kk + 16, cols] = hi
                    else:
                        W[b, kk:kk + 16, 0:LANES] = hi
                        W[b, kk:kk + 16, LANES:2 * LANES] = (w - hi.astype(f32)).astype(bf16)

    for lev in range(3):
        n = nx >> (lev + 1)
        scale = 2.0 ** (-12 * (lev + 1))
        entries = []
        for r, c in [(0, n), (7, -1)] + ([(1, n + 1)] if HI[lev] == 2 else []):
            for k, val in full[lev][c].items():
                entries.append((r, k if k < LANES // 2 else k - nx + LANES, val * scale))
        x = spots(entries)
        hi, lo = split2(x)
        both = jnp.concatenate([hi.astype(f32), lo.astype(f32)], axis=0)
        WG[16 * lev:16 * lev + 16] = both.astype(bf16)

    def z_block(lt, r, base):
        cols = pl.ds(pl.multiple_of(lt * LANES, LANES), LANES)
        x = [v[i, r:r + 8, cols] for i in range(nz)]
        for s in range(ext[0]):
            o = s - 1
            y = partial_conv(lambda i: x[i], o, 0, nz)
            if o < 0:
                y = y * fz_lo
            elif o >= m[0]:
                y = y * fz_hi
            Z[pl.ds(base + s * ZP + r + 2, 8)] = y

    def zrow(n, mz):
        row = lax.broadcasted_iota(jnp.int32, (n, LANES), 0)
        return jnp.where(row == 0, fz_lo, jnp.where(row > mz, fz_hi, 1.0))

    def edge(lt, base):
        src = {}

        def zy(y):
            if y not in src:
                src[y] = Z[pl.ds(base + y + 2, ext[0], ZP)]
            return src[y]
        f2, f3 = zrow(ext[1], m[1]), zrow(ext[2], m[2])
        n1, n2, n3 = rw
        rows1 = [-1, 0, 1, 2] + list(range(n1 - 6, n1 + 1))
        a2z = {}
        for k, e in enumerate(rows1):
            x = partial_conv(zy, e, 0, ny)
            EA1[k * E1P + 3:k * E1P + 3 + ext[0]] = x
            if e == -1:
                YG[0:ext[0]] = x
            elif e == n1:
                YG[16:16 + ext[0]] = x
        for k, e in enumerate(rows1):
            a2z[e] = conv(lambda j: EA1[pl.ds(k * E1P + 2 + j, ext[1], 2)]) * f2
        at = pl.multiple_of(lt * 16, 8)
        EG2[pl.ds(at, ext[1])] = a2z[-1]
        EG2[pl.ds(at + 8, ext[1])] = a2z[n1]
        rows2 = [-1, 0, n2 - 2, n2 - 1, n2, n2 + 1]
        a3z = {}
        for k, e in enumerate(rows2):
            x = partial_conv(lambda i: a2z[i], e, -1, n1 + 1)
            EA2[k * E2P + 3:k * E2P + 3 + ext[1]] = x
            if e in (-1, n2, n2 + 1):
                r = 32 + 8 * (0, n2, n2 + 1).index(max(e, 0))
                YG[r:r + ext[1]] = x
        for k, e in enumerate(rows2):
            a3z[e] = conv(lambda j: EA2[pl.ds(k * E2P + 2 + j, ext[2], 2)]) * f3
        EG3[pl.ds(at, ext[2])] = a3z[-1]
        EG3[pl.ds(at + 8, ext[2])] = a3z[n2]
        for k, e in enumerate((-1, n3, n3 + 1)):
            x = partial_conv(lambda i: a3z[i], e, -1, n2 + 2)
            YG[64 + 8 * k:64 + 8 * k + ext[2]] = x
        cols = pl.ds(pl.multiple_of(lt * LANES, LANES), LANES)
        for lev in range(3):
            hi, mid = split2(YG[32 * lev:32 * lev + 32])
            YX[64 * lev:64 * lev + 32, cols] = hi
            YX[64 * lev + 32:64 * lev + 64, cols] = mid

    order3 = list(range(1, ext[2])) + [0]

    def main(lt, base):
        cols = pl.ds(pl.multiple_of(lt * LANES, LANES), LANES)
        at = pl.multiple_of(lt * 16, 8)
        A2Z[pl.ds(1, ext[1], P2)] = EG2[pl.ds(at, ext[1])] * fy_lo
        A2Z[pl.ds(rw[0] + 2, ext[1], P2)] = EG2[pl.ds(at + 8, ext[1])] * fy_hi
        A3Z[pl.ds(1, ext[2], P3)] = EG3[pl.ds(at, ext[2])] * fy_lo
        A3Z[pl.ds(rw[1] + 2, ext[2], P3)] = EG3[pl.ds(at + 8, ext[2])] * fy_hi

        def reduce_sections(x, lev):
            for s in range(ext[lev]):
                y = partial_conv(lambda i: x[i + 1], s - 1, -1, len(x) - 1)
                if s == 0:
                    y = y * fz_lo
                elif s > m[lev]:
                    y = y * fz_hi
                yield s, y

        for q in range(0, rw[0], 16):
            x = []
            for s in range(ext[0]):
                half = [conv(lambda j: Z[pl.ds(base + s * ZP + 2 * (q + h) + 2 + j, 8, 2)])
                        for h in (0, 8)]
                y = jnp.concatenate(half, axis=0)
                hi, mid = split2(y)
                r = s * rw[0] + q
                LX1[r:r + 16, cols] = hi
                LX1[ext[0] * rw[0] + r:ext[0] * rw[0] + r + 16, cols] = mid
                x.append(y)
            for s, y in reduce_sections(x, 1):
                A2Z[s * P2 + q + 2:s * P2 + q + 18] = y
        for q in range(0, rw[1], 16):
            x = []
            for s in range(ext[1]):
                half = [conv(lambda j: A2Z[pl.ds(s * P2 + 2 * (q + h) + 2 + j, 8, 2)])
                        for h in (0, 8)]
                y = jnp.concatenate(half, axis=0)
                hi, mid = split2(y)
                r = s * rw[1] + q
                LX2[r:r + 16, cols] = hi
                LX2[ext[1] * rw[1] + r:ext[1] * rw[1] + r + 16, cols] = mid
                x.append(y)
            for s, y in reduce_sections(x, 2):
                A3Z[s * P3 + q + 2:s * P3 + q + 18] = y
        x = {}
        for s in range(ext[2]):
            x[s] = conv(lambda j: A3Z[pl.ds(s * P3 + 2 + j, 8, 2)])
        n = LX3.shape[0] // 2
        for i in range(0, n // 8, 2):
            pair = [x[order3[k]] if k < ext[2] else zero for k in (i, i + 1)]
            hi, mid = split2(jnp.concatenate(pair, axis=0))
            LX3[8 * i:8 * i + 16, cols] = hi
            LX3[n + 8 * i:n + 8 * i + 16, cols] = mid

    def columns(lev, rows_of):
        W = (W1, W2, W3)[lev]
        for b, lts in blocks_of(lev, nt):
            x = rows_of(slice(lts[0] * LANES, (lts[-1] + 1) * LANES))
            d = jnp.dot(x, W[b, 0:len(lts) * LANES], preferred_element_type=f32)
            n = x.shape[0] // 2
            d = d[0:n] + d[n:2 * n]
            if lev == 2:
                yield b, d[:, 0:LANES] + d[:, LANES:2 * LANES]
            else:
                for part in range(WIDE[lev] // LANES):
                    yield (b * (WIDE[lev] // LANES) + part,
                           d[:, part * LANES:(part + 1) * LANES])

    lane_k = lax.broadcasted_iota(jnp.int32, (16, LANES), 1) < LANES // 2

    def ends(ref, r, n):
        pieces = []
        for i in range(r, r + n, 16):
            a = ref[i:i + 16, 0:LANES].astype(f32)
            c = ref[i:i + 16, (nt - 1) * LANES:nt * LANES].astype(f32)
            pieces.append(jnp.where(lane_k, a, c).astype(bf16))
        return pieces

    def spill_columns(parts):
        his, mids = [], []
        for tile in parts:
            used = 0
            for lev, ref, r, n, off in tile:
                his += ends(ref, r, n)
                mids += ends(ref, r + off, n)
                used += n
            if used < LANES:
                fill = jnp.zeros((LANES - used, LANES), bf16)
                his.append(fill)
                mids.append(fill)
        rhs = jnp.concatenate(
            [jnp.concatenate(his, axis=0), jnp.concatenate(mids, axis=0)], axis=1)
        w = WG[...]
        lhs = jnp.concatenate([w, w], axis=1)
        d = lax.dot_general(lhs, rhs, (((1,), (1,)), ((), ())), preferred_element_type=f32)
        for i, tile in enumerate(parts):
            out, start = None, 0
            for lev, ref, r, n, off in tile:
                cols = slice(i * LANES, (i + 1) * LANES)
                x = d[16 * lev:16 * lev + 8, cols] + d[16 * lev + 8:16 * lev + 16, cols]
                out = x if out is None else jnp.where(lane >= start, x, out)
                start += n
            yield out

    sent = []

    def send(steps, src, dst):
        at = len(sent)
        copy = pltpu.make_async_remote_copy(
            src_ref=src, dst_ref=dst, send_sem=send_sem.at[at], recv_sem=recv_sem.at[at],
            device_id=device(steps), device_id_type=MESH)

        @pl.when(exists(steps))
        def _():
            copy.start()
        sent.append((steps, copy))

    for c in loads[0:2]:
        c.wait()

    @pl.loop(0, nt)
    def _(lt):
        base = lt * (ext[0] * ZP)
        for r in [0] + list(range(high, ny, 8)):
            z_block(lt, r, base)
        edge(lt, base)

    for lev in range(3):
        for t, d in columns(lev, lambda cols: YX[64 * lev:64 * lev + 64, cols]):
            DS[32 * t:32 * t + 32] = d
            e, mm, h = 16 if lev == 0 else 8, m[lev], HI[lev]
            for side in (0, 1):
                for k in range(h if side else 1):
                    r = 32 * t + e * (side + k)
                    slot = k * tiles[lev] + t
                    to = rowmap.own[lev] + slot * mm
                    YS[side, to:to + mm] = DS[r + 1:r + 1 + mm]
                    to = rowmap.hi[lev] + slot * h
                    YS[side, to:to + h] = DS[r + 1 + mm:r + 1 + mm + h]
                    to = rowmap.lo[lev] + slot
                    YS[side, to:to + 1] = DS[r:r + 1]
    spill = spill_columns([[(lev, YX, 64 * lev, 32, 32) for lev in range(3)]])
    XS[5] = next(spill)

    pl.semaphore_wait(barrier, sum(exists(p).astype(jnp.int32) for p in peers))
    segments = ((0, 0, rowmap.n_own), (1, rowmap.n_own, rowmap.n_hi),
                (-1, rowmap.n_own + rowmap.n_hi, rowmap.n_lo))

    def steps_of(dx, dy, dz):
        return {a: d for a, d in (("gz", dz), ("gy", dy), ("gx", dx)) if d}

    for dx in (1, -1):
        for dy in (1, -1):
            for dz in (0, 1, -1):
                slot = 5 + 3 * (dy < 0) + (0, 1, -1).index(dz)
                send(steps_of(dx, dy, dz), XS.at[5], XR.at[int(dx < 0), slot])
    for dy in (1, -1):
        side = int(dy > 0)
        for dz, at, n in segments:
            send(steps_of(0, dy, dz), YS.at[side, pl.ds(at, n)],
                 YR.at[int(dy < 0), pl.ds(at, n)])

    loads[2].wait()

    def tile_main(lt):
        base = lt * (ext[0] * ZP)
        for r in range(low, high, 8):
            z_block(lt, r, base)
        main(lt, base)

    @pl.loop(0, 2)
    def _(i):
        tile_main(i * (nt - 1))

    o1, o2 = ext[0] * rw[0], ext[1] * rw[1]
    o3 = LX3.shape[0] // 2
    own = [(0, LX1, rw[0] * (1 + i), LANES, o1) for i in range(0, m[0], LANES // rw[0])]
    parts = [[p] for p in own]
    parts.append([(1, LX2, rw[1], m[1] * rw[1], o2), (2, LX3, 0, m[2] * rw[2], o3)])
    parts.append([(0, LX1, rw[0] * (1 + m[0]), rw[0], o1),
                  (1, LX2, rw[1] * (1 + m[1]), 2 * rw[1], o2), (2, LX3, 16, 16, o3)])
    parts.append([(0, LX1, 0, rw[0], o1), (1, LX2, 0, rw[1], o2), (2, LX3, 32, 16, o3)])
    for i, x in enumerate(spill_columns(parts)):
        XS[i] = x
    for dx in (1, -1):
        side = int(dx < 0)
        send(steps_of(dx, 0, 0), XS.at[pl.ds(0, 3)], XR.at[side, pl.ds(0, 3)])
        send(steps_of(dx, 0, 1), XS.at[3], XR.at[side, 3])
        send(steps_of(dx, 0, -1), XS.at[4], XR.at[side, 4])

    @pl.loop(1, nt - 1)
    def _(lt):
        tile_main(lt)

    zat = [[0, 0, 0], [0, 0, 0]]
    at = [0, 0]
    for lev in range(3):
        for side in (0, 1):
            zat[side][lev] = at[side]
            at[side] += (HI[lev] if side else 1) * tiles[lev] * rw[lev]
    for lev, LX in ((0, LX1), (1, LX2), (2, LX3)):
        n, r = rw[lev], tiles[lev]
        for t, d in columns(lev, lambda cols: LX[:, cols]):
            for s in range(ext[lev]):
                i = order3.index(s) if lev == 2 else s
                x = d[i * n:(i + 1) * n]
                if s == 0:
                    to = zat[0][lev] + t * n
                    ZS[0, to:to + n] = x
                elif s > m[lev]:
                    to = zat[1][lev] + ((s - 1 - m[lev]) * r + t) * n
                    ZS[1, to:to + n] = x
                else:
                    to = ((s - 1) * r + t) * n
                    outs[lev][to:to + n] = x
    for dz in (1, -1):
        side = int(dz > 0)
        send(steps_of(0, 0, dz), ZS.at[side], ZR.at[side])

    def wait_all(which):
        for steps, copy in sent:
            if which(steps):
                @pl.when(exists({a: -d for a, d in steps.items()}))
                def _():
                    copy.wait_recv()

    wait_all(lambda s: "gx" not in s and "gy" in s)
    for lev in range(3):
        o, n, r, mm = outs[lev], rw[lev], tiles[lev], m[lev]
        pitch = r * n
        for side in (0, 1):
            for k in range(1 if side else HI[lev]):
                y = n - 1 if side else k
                for t in range(r):
                    slot = k * r + t
                    at = rowmap.own[lev] + slot * mm
                    x = YR[side, at:at + mm]
                    h = HI[lev]
                    at = rowmap.hi[lev] + slot * h
                    up = YR[side, at:at + h]
                    at = rowmap.lo[lev] + slot
                    down = YR[side, at:at + 1]
                    here = pl.ds(t * n + y, mm, pitch)
                    o[here] = o[here] + x
                    here = pl.ds(t * n + y, h, pitch) if h > 1 else pl.ds(t * n + y, 1)
                    o[here] = o[here] + up
                    here = pl.ds((mm - 1) * pitch + t * n + y, 1)
                    o[here] = o[here] + down

    wait_all(lambda s: "gx" in s and "gy" not in s)

    def unpack(lo, hi):
        x = jnp.concatenate([lo, jnp.zeros((LANES - 16, LANES), f32), hi], axis=0)
        return x.T

    def add_columns(lev, here, x):
        o = outs[lev]
        lanes = lax.broadcasted_iota(jnp.int32, x.shape, 1)
        a, c = jnp.where(lanes < 2, x, 0.0), jnp.where(lanes == LANES - 1, x, 0.0)
        for t, add in ((0, a), (tiles[lev] - 1, c)):
            if tiles[lev] == 1:
                if t == 0 and add is a:
                    o[here(0)] = o[here(0)] + (a + c)
                return
            o[here(t)] = o[here(t)] + add

    def section(lev, z, x):
        n = rw[lev]
        add_columns(lev, lambda t: pl.ds((z * tiles[lev] + t) * n, n), x)

    for i in range(len(own)):
        x = unpack(XR[0, i], XR[1, i])
        for j in range(LANES // rw[0]):
            section(0, i * (LANES // rw[0]) + j, x[j * rw[0]:(j + 1) * rw[0]])
    x = unpack(XR[0, 2], XR[1, 2])
    for z in range(m[1]):
        section(1, z, x[z * rw[1]:(z + 1) * rw[1]])
    at = m[1] * rw[1]
    for z in range(m[2]):
        section(2, z, x[at + z * rw[2]:at + (z + 1) * rw[2]])
    x = unpack(XR[0, 3], XR[1, 3])
    at = 0
    for lev in range(3):
        for z in range(HI[lev]):
            section(lev, z, x[at:at + rw[lev]])
            at += rw[lev]
    x = unpack(XR[0, 4], XR[1, 4])
    at = 0
    for lev in range(3):
        section(lev, m[lev] - 1, x[at:at + rw[lev]])
        at += rw[lev]

    wait_all(lambda s: "gx" in s and "gy" in s)
    lane96 = lane % 32
    kind_s = jnp.where(lane < 32, lane % 16, lane % 8)
    is_up = lane96 >= jnp.where(lane < 32, 16, 8)
    top = jnp.where(lane < 32, m[0], jnp.where(lane < 64, m[1], m[2]))

    def merge(side):
        total = jnp.zeros((8, LANES), f32)
        for j, up in ((0, True), (1, False)):
            for i in range(3):
                x = XR[side, 5 + 3 * j + i]
                if i == 0:
                    ok = jnp.logical_and(kind_s >= 1, kind_s <= top)
                elif i == 1:
                    ok = kind_s > top
                else:
                    ok = kind_s == 0
                ok = jnp.logical_and(ok, is_up if up else lane96 < jnp.where(lane < 32, 16, 8))
                total = jnp.where(ok, x, total)
        return total

    x = unpack(merge(0), merge(1))
    DS[0:LANES] = x
    for lev in range(3):
        n, r, mm, h = rw[lev], tiles[lev], m[lev], HI[lev]
        pitch = r * n
        e = 16 if lev == 0 else 8
        for side in (0, 1):
            for k in range(h if side else 1):
                at = 32 * lev + e * (side + k)
                y = k if side else n - 1
                add_columns(lev, lambda t: pl.ds(t * n + y, mm, pitch), DS[at + 1:at + 1 + mm])
                add_columns(
                    lev, lambda t: pl.ds(t * n + y, h, pitch) if h > 1 else pl.ds(t * n + y, 1),
                    DS[at + 1 + mm:at + 1 + mm + h])
                add_columns(lev, lambda t: pl.ds((mm - 1) * pitch + t * n + y, 1), DS[at:at + 1])

    wait_all(lambda s: "gx" not in s and "gy" not in s)
    for lev in range(3):
        o, n, r = outs[lev], rw[lev], tiles[lev]
        cnt = HI[lev] * r * n
        o[0:cnt] = o[0:cnt] + ZR[1, zat[1][lev]:zat[1][lev] + cnt]
        cnt, start = r * n, (m[lev] - 1) * r * n
        o[start:start + cnt] = o[start:start + cnt] + ZR[0, zat[0][lev]:zat[0][lev] + cnt]

    for steps, copy in sent:
        @pl.when(exists(steps))
        def _():
            copy.wait_send()


def write_out(a1, a2, a3, out1, out2, out3, sem):
    copies = []
    for src, dst in ((a1, out1), (a2, out2), (a3, out3)):
        for t in range(src.shape[1]):
            copies.append(pltpu.make_async_copy(
                src.at[:, t], dst.at[:, :, pl.ds(t * LANES, LANES)], sem.at[len(copies)]))
    for c in copies:
        c.start()
    for c in copies:
        c.wait()


def on_device(sizes, volume):
    nz, ny, nx = volume.shape
    nt = nx // LANES
    V = pltpu.VMEM
    m = [nz >> (l + 1) for l in range(3)]
    rw = [ny >> (l + 1) for l in range(3)]
    tiles = [nt >> (l + 1) for l in range(3)]
    ext = [m[l] + 1 + HI[l] for l in range(3)]
    ZP, P2, P3 = ny + 3, rw[0] + 3, rw[1] + 3
    E1P, E2P = 2 * ext[1] + 3, 2 * ext[2] + 3
    rowmap = Rows(m, tiles)
    n3 = -(-ext[2] * rw[2] // 16) * 16
    zrows = sum(HI[l] * tiles[l] * rw[l] for l in range(3))
    dma = pltpu.SemaphoreType.DMA
    hbm = pl.BlockSpec(memory_space=pltpu.HBM)
    vmem = pl.BlockSpec(memory_space=pltpu.VMEM)

    def flat(n):
        return V((-(-n // 8) * 8, LANES), f32)

    def weights(lev):
        found = blocks_of(lev, nt)
        depth = max(len(lts) for b, lts in found) * LANES
        return V((len(found), depth, 256 if lev == 2 else WIDE[lev]), bf16)

    volume = pltpu.with_memory_space_constraint(volume, pltpu.HBM)
    results = pl.pallas_call(
        functools.partial(kernel, sizes, (nz, ny, nt)),
        out_shape=tuple(V((m[l] * tiles[l] * rw[l], LANES), f32) for l in range(3)),
        in_specs=[hbm],
        out_specs=(vmem, vmem, vmem),
        scratch_shapes=[
            V((nz, ny, nx), f32),
            flat(nt * ext[0] * ZP), flat(ext[1] * P2), flat(ext[2] * P3),
            flat(11 * E1P), flat(6 * E2P), flat(16 * nt), flat(16 * nt), flat(96),
            V((192, nx), bf16),
            V((2 * ext[0] * rw[0], nx), bf16), V((2 * ext[1] * rw[1], nx), bf16),
            V((2 * n3, nx), bf16),
            weights(0), weights(1), weights(2), V((48, LANES), bf16),
            flat(LANES), V((2, rowmap.total, LANES), f32), V((2, rowmap.total, LANES), f32),
            V((6, 8, LANES), f32), V((2, 11, 8, LANES), f32),
            V((2, zrows, LANES), f32), V((2, zrows, LANES), f32),
            dma((3,)), dma((26,)), dma((26,)),
        ],
        compiler_params=pltpu.CompilerParams(
            collective_id=0, has_side_effects=True, vmem_limit_bytes=40 << 20),
        name="pyramid",
    )(volume)
    results = [x.reshape(m[l], tiles[l], rw[l], LANES) for l, x in enumerate(results)]
    return pl.pallas_call(
        write_out,
        out_shape=tuple(
            jax.ShapeDtypeStruct((nz >> l, ny >> l, nx >> l), f32) for l in (1, 2, 3)),
        in_specs=[vmem] * 3,
        out_specs=(hbm, hbm, hbm),
        scratch_shapes=[dma((sum(tiles),))],
        compiler_params=pltpu.CompilerParams(vmem_limit_bytes=4 << 20),
        name="write_out",
    )(*results)


def solution(mesh):
    sizes = {a: mesh.shape[a] for a in AXES}
    spec = P(*AXES)
    return jax.shard_map(
        functools.partial(on_device, sizes), mesh=mesh, in_specs=(spec,),
        out_specs=(spec, spec, spec), check_vma=False)
```

```python
import functools
import itertools

import jax
import jax.numpy as jnp
import numpy as np
from jax import lax
from jax.experimental import pallas as pl
from jax.experimental.pallas import tpu as pltpu
from jax.sharding import PartitionSpec as P

LANES = 128
MESH = pl.DeviceIdType.MESH
AXES = ("gz", "gy", "gx")
TAPS = {-2: 1, -1: 4, 0: 6, 1: 4, 2: 1}
HI = (1, 2, 2)
WIDE = (256, 128, 128)
f32, bf16 = jnp.float32, jnp.bfloat16


def chain(n, lo, hi):
    prev = {i: {i: 1} for i in range(n)}
    levels = []
    for lev in range(3):
        n //= 2
        cur = {}
        for o in range(-1 if lo else 0, n + (HI[lev] if hi else 0)):
            col = {}
            for j, w in TAPS.items():
                for k, v in prev.get(2 * o + j, {}).items():
                    col[k] = col.get(k, 0) + w * v
            cur[o] = col
        levels.append(cur)
        prev = cur
    return levels


def split2(x):
    hi = x.astype(bf16)
    return hi, (x - hi.astype(f32)).astype(bf16)


def blocks_of(lev, nt):
    per = WIDE[lev] * (2 << lev) // LANES
    return [(b, list(range(max(per * b - 1, 0), min(per * (b + 1) + 1, nt))))
            for b in range(nt // per)]


class Rows:
    def __init__(self, m, tiles):
        self.own, at = [], 0
        for lev in range(3):
            self.own.append(at)
            at += HI[lev] * tiles[lev] * m[lev]
        self.n_own = -(-at // 8) * 8
        self.hi, at = [], self.n_own
        for lev in range(3):
            self.hi.append(at)
            at += HI[lev] * tiles[lev] * HI[lev]
        self.n_hi = -(-(at - self.n_own) // 8) * 8
        self.lo, at = [], self.n_own + self.n_hi
        for lev in range(3):
            self.lo.append(at)
            at += HI[lev] * tiles[lev]
        self.n_lo = -(-(at - self.n_own - self.n_hi) // 8) * 8
        self.total = self.n_own + self.n_hi + self.n_lo


def conv(load):
    return (load(-2) + load(2)) + 4.0 * (load(-1) + load(1)) + 6.0 * load(0)


def partial_conv(load, o, lo, hi):
    have = [j for j in TAPS if lo <= 2 * o + j < hi]
    if len(have) == 5:
        return conv(lambda j: load(2 * o + j))
    total = None
    for j in have:
        term = load(2 * o + j)
        if TAPS[j] != 1:
            term = float(TAPS[j]) * term
        total = term if total is None else total + term
    return total


def kernel(sizes, dims, vol, out1, out2, out3,
           v, Z, A2Z, A3Z, EA1, EA2, EG2, EG3, YG, YX, LX1, LX2, LX3,
           W1, W2, W3, WG, DS, YS, YR, XS, XR, ZS, ZR,
           load_sem, send_sem, recv_sem):
    nz, ny, nt = dims
    m = [nz >> 1, nz >> 2, nz >> 3]
    rw = [ny >> 1, ny >> 2, ny >> 3]
    ext = [m[l] + 1 + HI[l] for l in range(3)]
    tiles = [nt >> 1, nt >> 2, nt >> 3]
    ZP, P2, P3 = ny + 3, rw[0] + 3, rw[1] + 3
    E1P, E2P = 2 * ext[1] + 3, 2 * ext[2] + 3
    rowmap = Rows(m, tiles)
    outs = (out1, out2, out3)

    idx = {a: lax.axis_index(a) for a in AXES}
    has, near = {}, {}
    for a in AXES:
        has[a, -1], has[a, 1] = idx[a] > 0, idx[a] < sizes[a] - 1
        near[a, -1] = jnp.maximum(idx[a] - 1, 0)
        near[a, 1] = jnp.minimum(idx[a] + 1, sizes[a] - 1)

    def exists(steps):
        found = None
        for a, d in steps.items():
            found = has[a, d] if found is None else jnp.logical_and(found, has[a, d])
        return found

    def device(steps):
        return {a: near[a, d] for a, d in steps.items()}

    def flag(a, d):
        return jnp.where(has[a, d], 1.0, 0.0).astype(f32)

    fz_lo, fz_hi = flag("gz", -1), flag("gz", 1)
    fy_lo, fy_hi = flag("gy", -1), flag("gy", 1)
    fx_lo, fx_hi = flag("gx", -1), flag("gx", 1)

    peers = []
    for dx, dy, dz in itertools.product((-1, 1, 0), (-1, 1, 0), (1, -1, 0)):
        p = {a: d for a, d in (("gz", dz), ("gy", dy), ("gx", dx)) if d}
        if p:
            peers.append(p)
    barrier = pltpu.get_barrier_semaphore()

    low, high = 8, ny - 16
    loads = []
    for i, (r0, rn) in enumerate(((0, low), (high, 16), (low, high - low))):
        c = pltpu.make_async_copy(
            vol.at[:, pl.ds(r0, rn), :], v.at[:, pl.ds(r0, rn), :], load_sem.at[i])
        c.start()
        loads.append(c)
    for p in peers:
        @pl.when(exists(p))
        def _():
            pl.semaphore_signal(barrier, inc=1, device_id=device(p), device_id_type=MESH)

    segments = ((0, 0, rowmap.n_own), (1, rowmap.n_own, rowmap.n_hi),
                (-1, rowmap.n_own + rowmap.n_hi, rowmap.n_lo))
    sent = []

    def message(steps, src, dst):
        at = len(sent)
        sent.append((steps, dst, pltpu.make_async_remote_copy(
            src_ref=src, dst_ref=dst, send_sem=send_sem.at[at], recv_sem=recv_sem.at[at],
            device_id=device(steps), device_id_type=MESH)))

    def steps_of(dx, dy, dz):
        return {a: d for a, d in (("gz", dz), ("gy", dy), ("gx", dx)) if d}

    for dx in (-1, 1):
        for dy in (-1, 1):
            for dz in (0, 1, -1):
                slot = 5 + 3 * (dy < 0) + (0, 1, -1).index(dz)
                message(steps_of(dx, dy, dz), XS.at[5], XR.at[int(dx < 0), slot])
    for dy in (-1, 1):
        for dz, at, n in segments:
            message(steps_of(0, dy, dz), YS.at[int(dy > 0), pl.ds(at, n)],
                    YR.at[int(dy < 0), pl.ds(at, n)])
    for dx in (-1, 1):
        side = int(dx < 0)
        message(steps_of(dx, 0, 0), XS.at[pl.ds(0, 3)], XR.at[side, pl.ds(0, 3)])
        message(steps_of(dx, 0, 1), XS.at[3], XR.at[side, 3])
        message(steps_of(dx, 0, -1), XS.at[4], XR.at[side, 4])
    for dz in (1, -1):
        side = int(dz > 0)
        message(steps_of(0, 0, dz), ZS.at[side], ZR.at[side])

    def start(which, when=None):
        for steps, dst, copy in sent:
            if which(steps):
                ok = exists(steps)

                @pl.when(ok if when is None else jnp.logical_and(ok, when))
                def _():
                    copy.start()

    for steps, dst, copy in sent:
        @pl.when(jnp.logical_not(exists({a: -d for a, d in steps.items()})))
        def _():
            dst[...] = jnp.zeros(dst.shape, f32)

    def with_rows(steps):
        return "gy" in steps

    def with_columns(steps):
        return "gx" in steps and "gy" not in steps

    def with_sections(steps):
        return "gx" not in steps and "gy" not in steps

    def meet():
        pl.semaphore_wait(barrier, sum(exists(p).astype(jnp.int32) for p in peers))

    first_tile = jnp.logical_not(jnp.logical_or(has["gx", -1], has["gy", -1]))
    later_tile = jnp.logical_or(has["gx", -1], has["gy", -1])

    zero = jnp.zeros((8, LANES), f32)

    def clear(ref, at, n):
        ref[at:at + n] = jnp.zeros((n, LANES), f32)

    clear(Z, 0, 2)

    @pl.loop(1, nt * ext[0])
    def _(i):
        Z[pl.ds(i * ZP - 1, 3)] = jnp.zeros((3, LANES), f32)
    clear(Z, nt * ext[0] * ZP - 1, 1)
    for s in range(ext[1]):
        clear(A2Z, s * P2, 1)
    for s in range(ext[2]):
        clear(A3Z, s * P3, 1)
    EA1[...] = jnp.zeros(EA1.shape, f32)
    EA2[...] = jnp.zeros(EA2.shape, f32)
    YG[...] = jnp.zeros(YG.shape, f32)

    row8 = lax.broadcasted_iota(jnp.int32, (8, LANES), 0)
    lane = lax.broadcasted_iota(jnp.int32, (8, LANES), 1)
    nx = nt * LANES
    full, no_lo, no_hi = chain(nx, True, True), chain(nx, False, True), chain(nx, True, False)

    def spots(entries):
        x = jnp.zeros((8, LANES), f32)
        for r, c, val in entries:
            x = jnp.where(jnp.logical_and(row8 == r, lane == c), float(val), x)
        return x

    def fixes(lev, other):
        found = {}
        for c in range(nx >> (lev + 1)):
            for k, val in full[lev][c].items():
                gone = val - other[lev].get(c, {}).get(k, 0)
                if gone:
                    found[k, c] = gone
        return found

    for lev, W in ((0, W1), (1, W2), (2, W3)):
        step = 2 << lev
        mid = (nx >> (lev + 1)) // 2
        tap = {k - step * mid: w for k, w in full[lev][mid].items()}
        reach = max(tap)
        scale = 2.0 ** (-12 * (lev + 1))
        signed = jnp.where(lane < LANES // 2, lane, lane - LANES)
        delta = row8 - step * signed
        dist = jnp.abs(delta)
        base = jnp.zeros((8, LANES), f32)
        for d in range(reach + 1):
            base = jnp.where(dist == d, tap[d] * scale, base)
        lo_fix, hi_fix = fixes(lev, no_lo), fixes(lev, no_hi)
        for b, lts in blocks_of(lev, nt):
            for part in range(WIDE[lev] // LANES):
                c0 = WIDE[lev] * b + LANES * part
                for kk in range(0, len(lts) * LANES, 16):
                    pieces = []
                    for k8 in (kk, kk + 8):
                        k = lts[0] * LANES + k8
                        first = -((-(k - reach)) // step) - c0
                        last = (k + 7 + reach) // step - c0
                        if last < 0 or first >= LANES:
                            pieces.append(zero)
                            continue
                        x = pltpu.roll(base, (k // step - c0) % LANES, 1)
                        if first < 0:
                            x = jnp.where(lane <= last, x, 0.0)
                        elif last >= LANES:
                            x = jnp.where(lane >= first, x, 0.0)
                        for fix, fl in ((lo_fix, fx_lo), (hi_fix, fx_hi)):
                            here = [(r - k, c - c0, val * scale) for (r, c), val in fix.items()
                                    if k <= r < k + 8 and c0 <= c < c0 + LANES]
                            if here:
                                x = x - (1.0 - fl) * spots(here)
                        pieces.append(x)
                    w = jnp.concatenate(pieces, axis=0)
                    hi = w.astype(bf16)
                    cols = slice(part * LANES, (part + 1) * LANES)
                    if lev < 2:
                        W[b, kk:kk + 16, cols] = hi
                    else:
                        W[b, kk:kk + 16, 0:LANES] = hi
                        W[b, kk:kk + 16, LANES:2 * LANES] = (w - hi.astype(f32)).astype(bf16)

    for lev in range(3):
        n = nx >> (lev + 1)
        scale = 2.0 ** (-12 * (lev + 1))
        entries = []
        for r, c in [(0, n), (7, -1)] + ([(1, n + 1)] if HI[lev] == 2 else []):
            for k, val in full[lev][c].items():
                entries.append((r, k if k < LANES // 2 else k - nx + LANES, val * scale))
        x = spots(entries)
        hi, lo = split2(x)
        both = jnp.concatenate([hi.astype(f32), lo.astype(f32)], axis=0)
        WG[16 * lev:16 * lev + 16] = both.astype(bf16)

    def z_block(lt, r, base):
        cols = pl.ds(pl.multiple_of(lt * LANES, LANES), LANES)
        x = [v[i, r:r + 8, cols] for i in range(nz)]
        for s in range(ext[0]):
            o = s - 1
            y = partial_conv(lambda i: x[i], o, 0, nz)
            if o < 0:
                y = y * fz_lo
            elif o >= m[0]:
                y = y * fz_hi
            Z[pl.ds(base + s * ZP + r + 2, 8)] = y

    def zrow(n, mz):
        row = lax.broadcasted_iota(jnp.int32, (n, LANES), 0)
        return jnp.where(row == 0, fz_lo, jnp.where(row > mz, fz_hi, 1.0))

    def edge(lt, base):
        src = {}

        def zy(y):
            if y not in src:
                src[y] = Z[pl.ds(base + y + 2, ext[0], ZP)]
            return src[y]
        f2, f3 = zrow(ext[1], m[1]), zrow(ext[2], m[2])
        n1, n2, n3 = rw
        rows1 = [-1, 0, 1, 2] + list(range(n1 - 6, n1 + 1))
        a2z = {}
        for k, e in enumerate(rows1):
            x = partial_conv(zy, e, 0, ny)
            EA1[k * E1P + 3:k * E1P + 3 + ext[0]] = x
            if e == -1:
                YG[0:ext[0]] = x
            elif e == n1:
                YG[16:16 + ext[0]] = x
        for k, e in enumerate(rows1):
            a2z[e] = conv(lambda j: EA1[pl.ds(k * E1P + 2 + j, ext[1], 2)]) * f2
        at = pl.multiple_of(lt * 16, 8)
        EG2[pl.ds(at, ext[1])] = a2z[-1]
        EG2[pl.ds(at + 8, ext[1])] = a2z[n1]
        rows2 = [-1, 0, n2 - 2, n2 - 1, n2, n2 + 1]
        a3z = {}
        for k, e in enumerate(rows2):
            x = partial_conv(lambda i: a2z[i], e, -1, n1 + 1)
            EA2[k * E2P + 3:k * E2P + 3 + ext[1]] = x
            if e in (-1, n2, n2 + 1):
                r = 32 + 8 * (0, n2, n2 + 1).index(max(e, 0))
                YG[r:r + ext[1]] = x
        for k, e in enumerate(rows2):
            a3z[e] = conv(lambda j: EA2[pl.ds(k * E2P + 2 + j, ext[2], 2)]) * f3
        EG3[pl.ds(at, ext[2])] = a3z[-1]
        EG3[pl.ds(at + 8, ext[2])] = a3z[n2]
        for k, e in enumerate((-1, n3, n3 + 1)):
            x = partial_conv(lambda i: a3z[i], e, -1, n2 + 2)
            YG[64 + 8 * k:64 + 8 * k + ext[2]] = x
        cols = pl.ds(pl.multiple_of(lt * LANES, LANES), LANES)
        for lev in range(3):
            hi, mid = split2(YG[32 * lev:32 * lev + 32])
            YX[64 * lev:64 * lev + 32, cols] = hi
            YX[64 * lev + 32:64 * lev + 64, cols] = mid

    order3 = list(range(1, ext[2])) + [0]

    def main(lt, base):
        cols = pl.ds(pl.multiple_of(lt * LANES, LANES), LANES)
        at = pl.multiple_of(lt * 16, 8)
        A2Z[pl.ds(1, ext[1], P2)] = EG2[pl.ds(at, ext[1])] * fy_lo
        A2Z[pl.ds(rw[0] + 2, ext[1], P2)] = EG2[pl.ds(at + 8, ext[1])] * fy_hi
        A3Z[pl.ds(1, ext[2], P3)] = EG3[pl.ds(at, ext[2])] * fy_lo
        A3Z[pl.ds(rw[1] + 2, ext[2], P3)] = EG3[pl.ds(at + 8, ext[2])] * fy_hi

        def reduce_sections(x, lev):
            for s in range(ext[lev]):
                y = partial_conv(lambda i: x[i + 1], s - 1, -1, len(x) - 1)
                if s == 0:
                    y = y * fz_lo
                elif s > m[lev]:
                    y = y * fz_hi
                yield s, y

        for q in range(0, rw[0], 16):
            x = []
            for s in range(ext[0]):
                half = [conv(lambda j: Z[pl.ds(base + s * ZP + 2 * (q + h) + 2 + j, 8, 2)])
                        for h in (0, 8)]
                y = jnp.concatenate(half, axis=0)
                hi, mid = split2(y)
                r = s * rw[0] + q
                LX1[r:r + 16, cols] = hi
                LX1[ext[0] * rw[0] + r:ext[0] * rw[0] + r + 16, cols] = mid
                x.append(y)
            for s, y in reduce_sections(x, 1):
                A2Z[s * P2 + q + 2:s * P2 + q + 18] = y
        for q in range(0, rw[1], 16):
            x = []
            for s in range(ext[1]):
                half = [conv(lambda j: A2Z[pl.ds(s * P2 + 2 * (q + h) + 2 + j, 8, 2)])
                        for h in (0, 8)]
                y = jnp.concatenate(half, axis=0)
                hi, mid = split2(y)
                r = s * rw[1] + q
                LX2[r:r + 16, cols] = hi
                LX2[ext[1] * rw[1] + r:ext[1] * rw[1] + r + 16, cols] = mid
                x.append(y)
            for s, y in reduce_sections(x, 2):
                A3Z[s * P3 + q + 2:s * P3 + q + 18] = y
        x = {}
        for s in range(ext[2]):
            x[s] = conv(lambda j: A3Z[pl.ds(s * P3 + 2 + j, 8, 2)])
        n = LX3.shape[0] // 2
        for i in range(0, n // 8, 2):
            pair = [x[order3[k]] if k < ext[2] else zero for k in (i, i + 1)]
            hi, mid = split2(jnp.concatenate(pair, axis=0))
            LX3[8 * i:8 * i + 16, cols] = hi
            LX3[n + 8 * i:n + 8 * i + 16, cols] = mid

    def columns(lev, rows_of):
        W = (W1, W2, W3)[lev]
        for b, lts in blocks_of(lev, nt):
            x = rows_of(slice(lts[0] * LANES, (lts[-1] + 1) * LANES))
            d = jnp.dot(x, W[b, 0:len(lts) * LANES], preferred_element_type=f32)
            n = x.shape[0] // 2
            d = d[0:n] + d[n:2 * n]
            if lev == 2:
                yield b, d[:, 0:LANES] + d[:, LANES:2 * LANES]
            else:
                for part in range(WIDE[lev] // LANES):
                    yield (b * (WIDE[lev] // LANES) + part,
                           d[:, part * LANES:(part + 1) * LANES])

    lane_k = lax.broadcasted_iota(jnp.int32, (16, LANES), 1) < LANES // 2

    def ends(ref, r, n):
        pieces = []
        for i in range(r, r + n, 16):
            a = ref[i:i + 16, 0:LANES].astype(f32)
            c = ref[i:i + 16, (nt - 1) * LANES:nt * LANES].astype(f32)
            pieces.append(jnp.where(lane_k, a, c).astype(bf16))
        return pieces

    def spill_columns(parts):
        his, mids = [], []
        for tile in parts:
            used = 0
            for lev, ref, r, n, off in tile:
                his += ends(ref, r, n)
                mids += ends(ref, r + off, n)
                used += n
            if used < LANES:
                fill = jnp.zeros((LANES - used, LANES), bf16)
                his.append(fill)
                mids.append(fill)
        rhs = jnp.concatenate(
            [jnp.concatenate(his, axis=0), jnp.concatenate(mids, axis=0)], axis=1)
        w = WG[...]
        lhs = jnp.concatenate([w, w], axis=1)
        d = lax.dot_general(lhs, rhs, (((1,), (1,)), ((), ())), preferred_element_type=f32)
        for i, tile in enumerate(parts):
            out, start = None, 0
            for lev, ref, r, n, off in tile:
                cols = slice(i * LANES, (i + 1) * LANES)
                x = d[16 * lev:16 * lev + 8, cols] + d[16 * lev + 8:16 * lev + 16, cols]
                out = x if out is None else jnp.where(lane >= start, x, out)
                start += n
            yield out

    for c in loads[0:2]:
        c.wait()

    @pl.loop(0, nt)
    def _(lt):
        base = lt * (ext[0] * ZP)
        for r in [0] + list(range(high, ny, 8)):
            z_block(lt, r, base)
        edge(lt, base)

    for lev in range(3):
        for t, d in columns(lev, lambda cols: YX[64 * lev:64 * lev + 64, cols]):
            DS[32 * t:32 * t + 32] = d
            e, mm, h = 16 if lev == 0 else 8, m[lev], HI[lev]
            for side in (0, 1):
                for k in range(h if side else 1):
                    r = 32 * t + e * (side + k)
                    slot = k * tiles[lev] + t
                    to = rowmap.own[lev] + slot * mm
                    YS[side, to:to + mm] = DS[r + 1:r + 1 + mm]
                    to = rowmap.hi[lev] + slot * h
                    YS[side, to:to + h] = DS[r + 1 + mm:r + 1 + mm + h]
                    to = rowmap.lo[lev] + slot
                    YS[side, to:to + 1] = DS[r:r + 1]
    spill = spill_columns([[(lev, YX, 64 * lev, 32, 32) for lev in range(3)]])
    XS[5] = next(spill)

    @pl.when(later_tile)
    def _():
        meet()
        start(with_rows)

    loads[2].wait()

    def tile_main(lt):
        base = lt * (ext[0] * ZP)
        for r in range(low, high, 8):
            z_block(lt, r, base)
        main(lt, base)

    @pl.loop(0, 2)
    def _(i):
        tile_main(i * (nt - 1))

    o1, o2 = ext[0] * rw[0], ext[1] * rw[1]
    o3 = LX3.shape[0] // 2
    own = [(0, LX1, rw[0] * (1 + i), LANES, o1) for i in range(0, m[0], LANES // rw[0])]
    parts = [[p] for p in own]
    parts.append([(1, LX2, rw[1], m[1] * rw[1], o2), (2, LX3, 0, m[2] * rw[2], o3)])
    parts.append([(0, LX1, rw[0] * (1 + m[0]), rw[0], o1),
                  (1, LX2, rw[1] * (1 + m[1]), 2 * rw[1], o2), (2, LX3, 16, 16, o3)])
    parts.append([(0, LX1, 0, rw[0], o1), (1, LX2, 0, rw[1], o2), (2, LX3, 32, 16, o3)])
    for i, x in enumerate(spill_columns(parts)):
        XS[i] = x
    start(with_columns, later_tile)

    @pl.loop(1, nt - 1)
    def _(lt):
        tile_main(lt)

    @pl.when(first_tile)
    def _():
        meet()
        start(with_rows)
        start(with_columns)

    zat = [[0, 0, 0], [0, 0, 0]]
    at = [0, 0]
    for lev in range(3):
        for side in (0, 1):
            zat[side][lev] = at[side]
            at[side] += (HI[lev] if side else 1) * tiles[lev] * rw[lev]
    for lev, LX in ((0, LX1), (1, LX2), (2, LX3)):
        n, r = rw[lev], tiles[lev]
        for t, d in columns(lev, lambda cols: LX[:, cols]):
            for s in range(ext[lev]):
                i = order3.index(s) if lev == 2 else s
                x = d[i * n:(i + 1) * n]
                if s == 0:
                    to = zat[0][lev] + t * n
                    ZS[0, to:to + n] = x
                elif s > m[lev]:
                    to = zat[1][lev] + ((s - 1 - m[lev]) * r + t) * n
                    ZS[1, to:to + n] = x
                else:
                    to = ((s - 1) * r + t) * n
                    outs[lev][to:to + n] = x
    start(with_sections)

    def wait_all(which):
        for steps, dst, copy in sent:
            if which(steps):
                @pl.when(exists({a: -d for a, d in steps.items()}))
                def _():
                    copy.wait_recv()

    wait_all(lambda s: "gx" not in s and "gy" not in s)
    for lev in range(3):
        o, n, r = outs[lev], rw[lev], tiles[lev]
        cnt = HI[lev] * r * n
        o[0:cnt] = o[0:cnt] + ZR[1, zat[1][lev]:zat[1][lev] + cnt]
        cnt, start = r * n, (m[lev] - 1) * r * n
        o[start:start + cnt] = o[start:start + cnt] + ZR[0, zat[0][lev]:zat[0][lev] + cnt]

    wait_all(lambda s: "gx" not in s and "gy" in s)
    for lev in range(3):
        o, n, r, mm = outs[lev], rw[lev], tiles[lev], m[lev]
        pitch = r * n
        for side in (0, 1):
            for k in range(1 if side else HI[lev]):
                y = n - 1 if side else k
                for t in range(r):
                    slot = k * r + t
                    at = rowmap.own[lev] + slot * mm
                    x = YR[side, at:at + mm]
                    h = HI[lev]
                    at = rowmap.hi[lev] + slot * h
                    up = YR[side, at:at + h]
                    at = rowmap.lo[lev] + slot
                    down = YR[side, at:at + 1]
                    here = pl.ds(t * n + y, mm, pitch)
                    o[here] = o[here] + x
                    here = pl.ds(t * n + y, h, pitch) if h > 1 else pl.ds(t * n + y, 1)
                    o[here] = o[here] + up
                    here = pl.ds((mm - 1) * pitch + t * n + y, 1)
                    o[here] = o[here] + down

    wait_all(lambda s: "gx" in s and "gy" not in s)

    def unpack(lo, hi):
        x = jnp.concatenate([lo, jnp.zeros((LANES - 16, LANES), f32), hi], axis=0)
        return x.T

    def add_columns(lev, here, x):
        o = outs[lev]
        lanes = lax.broadcasted_iota(jnp.int32, x.shape, 1)
        a, c = jnp.where(lanes < 2, x, 0.0), jnp.where(lanes == LANES - 1, x, 0.0)
        for t, add in ((0, a), (tiles[lev] - 1, c)):
            if tiles[lev] == 1:
                if t == 0 and add is a:
                    o[here(0)] = o[here(0)] + (a + c)
                return
            o[here(t)] = o[here(t)] + add

    def section(lev, z, x):
        n = rw[lev]
        add_columns(lev, lambda t: pl.ds((z * tiles[lev] + t) * n, n), x)

    for i in range(len(own)):
        x = unpack(XR[0, i], XR[1, i])
        for j in range(LANES // rw[0]):
            section(0, i * (LANES // rw[0]) + j, x[j * rw[0]:(j + 1) * rw[0]])
    x = unpack(XR[0, 2], XR[1, 2])
    for z in range(m[1]):
        section(1, z, x[z * rw[1]:(z + 1) * rw[1]])
    at = m[1] * rw[1]
    for z in range(m[2]):
        section(2, z, x[at + z * rw[2]:at + (z + 1) * rw[2]])
    x = unpack(XR[0, 3], XR[1, 3])
    at = 0
    for lev in range(3):
        for z in range(HI[lev]):
            section(lev, z, x[at:at + rw[lev]])
            at += rw[lev]
    x = unpack(XR[0, 4], XR[1, 4])
    at = 0
    for lev in range(3):
        section(lev, m[lev] - 1, x[at:at + rw[lev]])
        at += rw[lev]

    wait_all(lambda s: "gx" in s and "gy" in s)
    lane96 = lane % 32
    kind_s = jnp.where(lane < 32, lane % 16, lane % 8)
    is_up = lane96 >= jnp.where(lane < 32, 16, 8)
    top = jnp.where(lane < 32, m[0], jnp.where(lane < 64, m[1], m[2]))

    def merge(side):
        total = jnp.zeros((8, LANES), f32)
        for j, up in ((0, True), (1, False)):
            for i in range(3):
                x = XR[side, 5 + 3 * j + i]
                if i == 0:
                    ok = jnp.logical_and(kind_s >= 1, kind_s <= top)
                elif i == 1:
                    ok = kind_s > top
                else:
                    ok = kind_s == 0
                ok = jnp.logical_and(ok, is_up if up else lane96 < jnp.where(lane < 32, 16, 8))
                total = jnp.where(ok, x, total)
        return total

    x = unpack(merge(0), merge(1))
    DS[0:LANES] = x
    for lev in range(3):
        n, r, mm, h = rw[lev], tiles[lev], m[lev], HI[lev]
        pitch = r * n
        e = 16 if lev == 0 else 8
        for side in (0, 1):
            for k in range(h if side else 1):
                at = 32 * lev + e * (side + k)
                y = k if side else n - 1
                add_columns(lev, lambda t: pl.ds(t * n + y, mm, pitch), DS[at + 1:at + 1 + mm])
                add_columns(
                    lev, lambda t: pl.ds(t * n + y, h, pitch) if h > 1 else pl.ds(t * n + y, 1),
                    DS[at + 1 + mm:at + 1 + mm + h])
                add_columns(lev, lambda t: pl.ds((mm - 1) * pitch + t * n + y, 1), DS[at:at + 1])

    for steps, dst, copy in sent:
        @pl.when(exists(steps))
        def _():
            copy.wait_send()


def write_out(a1, a2, a3, out1, out2, out3, sem):
    copies = []
    for src, dst in ((a1, out1), (a2, out2), (a3, out3)):
        for t in range(src.shape[1]):
            copies.append(pltpu.make_async_copy(
                src.at[:, t], dst.at[:, :, pl.ds(t * LANES, LANES)], sem.at[len(copies)]))
    for c in copies:
        c.start()
    for c in copies:
        c.wait()


def on_device(sizes, volume):
    nz, ny, nx = volume.shape
    nt = nx // LANES
    V = pltpu.VMEM
    m = [nz >> (l + 1) for l in range(3)]
    rw = [ny >> (l + 1) for l in range(3)]
    tiles = [nt >> (l + 1) for l in range(3)]
    ext = [m[l] + 1 + HI[l] for l in range(3)]
    ZP, P2, P3 = ny + 3, rw[0] + 3, rw[1] + 3
    E1P, E2P = 2 * ext[1] + 3, 2 * ext[2] + 3
    rowmap = Rows(m, tiles)
    n3 = -(-ext[2] * rw[2] // 16) * 16
    zrows = sum(HI[l] * tiles[l] * rw[l] for l in range(3))
    dma = pltpu.SemaphoreType.DMA
    hbm = pl.BlockSpec(memory_space=pltpu.HBM)
    vmem = pl.BlockSpec(memory_space=pltpu.VMEM)

    def flat(n):
        return V((-(-n // 8) * 8, LANES), f32)

    def weights(lev):
        found = blocks_of(lev, nt)
        depth = max(len(lts) for b, lts in found) * LANES
        return V((len(found), depth, 256 if lev == 2 else WIDE[lev]), bf16)

    volume = pltpu.with_memory_space_constraint(volume, pltpu.HBM)
    results = pl.pallas_call(
        functools.partial(kernel, sizes, (nz, ny, nt)),
        out_shape=tuple(V((m[l] * tiles[l] * rw[l], LANES), f32) for l in range(3)),
        in_specs=[hbm],
        out_specs=(vmem, vmem, vmem),
        scratch_shapes=[
            V((nz, ny, nx), f32),
            flat(nt * ext[0] * ZP), flat(ext[1] * P2), flat(ext[2] * P3),
            flat(11 * E1P), flat(6 * E2P), flat(16 * nt), flat(16 * nt), flat(96),
            V((192, nx), bf16),
            V((2 * ext[0] * rw[0], nx), bf16), V((2 * ext[1] * rw[1], nx), bf16),
            V((2 * n3, nx), bf16),
            weights(0), weights(1), weights(2), V((48, LANES), bf16),
            flat(LANES), V((2, rowmap.total, LANES), f32), V((2, rowmap.total, LANES), f32),
            V((6, 8, LANES), f32), V((2, 11, 8, LANES), f32),
            V((2, zrows, LANES), f32), V((2, zrows, LANES), f32),
            dma((3,)), dma((26,)), dma((26,)),
        ],
        compiler_params=pltpu.CompilerParams(
            collective_id=0, has_side_effects=True, vmem_limit_bytes=40 << 20),
        name="pyramid",
    )(volume)
    results = [x.reshape(m[l], tiles[l], rw[l], LANES) for l, x in enumerate(results)]
    return pl.pallas_call(
        write_out,
        out_shape=tuple(
            jax.ShapeDtypeStruct((nz >> l, ny >> l, nx >> l), f32) for l in (1, 2, 3)),
        in_specs=[vmem] * 3,
        out_specs=(hbm, hbm, hbm),
        scratch_shapes=[dma((sum(tiles),))],
        compiler_params=pltpu.CompilerParams(vmem_limit_bytes=4 << 20),
        name="write_out",
    )(*results)


def solution(mesh):
    sizes = {a: mesh.shape[a] for a in AXES}
    spec = P(*AXES)
    return jax.shard_map(
        functools.partial(on_device, sizes), mesh=mesh, in_specs=(spec,),
        out_specs=(spec, spec, spec), check_vma=False)
```

```python
import functools
import itertools

import jax
import jax.numpy as jnp
import numpy as np
from jax import lax
from jax.experimental import pallas as pl
from jax.experimental.pallas import tpu as pltpu
from jax.sharding import PartitionSpec as P

LANES = 128
MESH = pl.DeviceIdType.MESH
AXES = ("gz", "gy", "gx")
TAPS = {-2: 1, -1: 4, 0: 6, 1: 4, 2: 1}
HI = (1, 2, 2)
WIDE = (256, 128, 128)
f32, bf16 = jnp.float32, jnp.bfloat16


def chain(n, lo, hi):
    prev = {i: {i: 1} for i in range(n)}
    levels = []
    for lev in range(3):
        n //= 2
        cur = {}
        for o in range(-1 if lo else 0, n + (HI[lev] if hi else 0)):
            col = {}
            for j, w in TAPS.items():
                for k, v in prev.get(2 * o + j, {}).items():
                    col[k] = col.get(k, 0) + w * v
            cur[o] = col
        levels.append(cur)
        prev = cur
    return levels


def split2(x):
    hi = x.astype(bf16)
    return hi, (x - hi.astype(f32)).astype(bf16)


def blocks_of(lev, nt):
    per = WIDE[lev] * (2 << lev) // LANES
    return [(b, list(range(max(per * b - 1, 0), min(per * (b + 1) + 1, nt))))
            for b in range(nt // per)]


class Rows:
    def __init__(self, m, tiles, up):
        count = HI if up else (1, 1, 1)
        self.own, at = [], 0
        for lev in range(3):
            self.own.append(at)
            at += count[lev] * tiles[lev] * m[lev]
        self.n_own = -(-at // 8) * 8
        self.hi, at = [], self.n_own
        for lev in range(3):
            self.hi.append(at)
            at += count[lev] * tiles[lev] * HI[lev]
        self.n_hi = -(-(at - self.n_own) // 8) * 8
        self.lo, at = [], self.n_own + self.n_hi
        for lev in range(3):
            self.lo.append(at)
            at += count[lev] * tiles[lev]
        self.n_lo = -(-(at - self.n_own - self.n_hi) // 8) * 8
        self.total = self.n_own + self.n_hi + self.n_lo


def aligned(i, n):
    return i * n if isinstance(i, int) else pl.multiple_of(i * n, n)


def conv(load):
    return (load(-2) + load(2)) + 4.0 * (load(-1) + load(1)) + 6.0 * load(0)


def partial_conv(load, o, lo, hi):
    have = [j for j in TAPS if lo <= 2 * o + j < hi]
    if len(have) == 5:
        return conv(lambda j: load(2 * o + j))
    total = None
    for j in have:
        term = load(2 * o + j)
        if TAPS[j] != 1:
            term = float(TAPS[j]) * term
        total = term if total is None else total + term
    return total


def kernel(sizes, dims, vol, out1, out2, out3,
           v, Z, A2Z, A3Z, EA1, EA2, EG2, EG3, YG, YX, LX1, LX2, LX3,
           W1, W2, W3, WG, DS, YS, YR, XS, XR, XQ, ZS, ZR,
           load_sem, send_sem, recv_sem, ready):
    nz, ny, nt = dims
    m = [nz >> 1, nz >> 2, nz >> 3]
    rw = [ny >> 1, ny >> 2, ny >> 3]
    ext = [m[l] + 1 + HI[l] for l in range(3)]
    tiles = [nt >> 1, nt >> 2, nt >> 3]
    ZP, P2, P3 = ny + 3, rw[0] + 3, rw[1] + 3
    E1P, E2P = 2 * ext[1] + 3, 2 * ext[2] + 3
    rowmaps = Rows(m, tiles, False), Rows(m, tiles, True)
    outs = (out1, out2, out3)

    idx = {a: lax.axis_index(a) for a in AXES}
    has, near = {}, {}
    for a in AXES:
        has[a, -1], has[a, 1] = idx[a] > 0, idx[a] < sizes[a] - 1
        near[a, -1] = jnp.maximum(idx[a] - 1, 0)
        near[a, 1] = jnp.minimum(idx[a] + 1, sizes[a] - 1)

    def exists(steps):
        found = None
        for a, d in steps.items():
            found = has[a, d] if found is None else jnp.logical_and(found, has[a, d])
        return found

    def device(steps):
        return {a: near[a, d] for a, d in steps.items()}

    def flag(a, d):
        return jnp.where(has[a, d], 1.0, 0.0).astype(f32)

    def upward(steps):
        return steps.get("gx") == 1 and steps.get("gy") == 1

    def downward(steps):
        return steps.get("gx") == -1 and steps.get("gy") == -1

    across = jnp.logical_and(idx["gy"] == sizes["gy"] // 2 - 1, has["gy", 1])
    below_across = idx["gy"] == sizes["gy"] // 2

    def near_by(steps):
        far = across if upward(steps) else below_across
        return jnp.logical_and(exists(steps), jnp.logical_not(far))

    fz_lo, fz_hi = flag("gz", -1), flag("gz", 1)
    fy_lo, fy_hi = flag("gy", -1), flag("gy", 1)
    fx_lo, fx_hi = flag("gx", -1), flag("gx", 1)

    peers = []
    for dx, dy, dz in itertools.product((-1, 1, 0), (-1, 1, 0), (1, -1, 0)):
        p = {a: d for a, d in (("gz", dz), ("gy", dy), ("gx", dx)) if d}
        if p:
            peers.append(p)
    barrier = pltpu.get_barrier_semaphore()

    low, high = 8, ny - 16
    loads = []
    tops, rest = ((0, low), (high, 16)), ((low, high - low),)
    ends_first = ((0, 1), (nt - 1, 1), (1, nt - 2))
    for rows, spans in ((tops, ends_first), (rest, ends_first)):
        for c0, cn in spans:
            for r0, rn in rows:
                here = (slice(None), pl.ds(r0, rn), pl.ds(c0 * LANES, cn * LANES))
                c = pltpu.make_async_copy(vol.at[here], v.at[here], load_sem.at[len(loads)])
                c.start()
                loads.append(c)
    for p in peers:
        if downward(p):
            continue

        @pl.when(exists(p))
        def _():
            pl.semaphore_signal(barrier, inc=1, device_id=device(p), device_id_type=MESH)

    sent = []

    def message(steps, src, dst):
        at = len(sent)
        sent.append((steps, dst, pltpu.make_async_remote_copy(
            src_ref=src, dst_ref=dst, send_sem=send_sem.at[at], recv_sem=recv_sem.at[at],
            device_id=device(steps), device_id_type=MESH)))

    def steps_of(dx, dy, dz):
        return {a: d for a, d in (("gz", dz), ("gy", dy), ("gx", dx)) if d}

    for dx in (-1, 1):
        for dy in (-1, 1):
            for dz in (0, 1, -1):
                slot = 5 + 3 * (dy < 0) + (0, 1, -1).index(dz)
                message(steps_of(dx, dy, dz), XS.at[5], XR.at[int(dx < 0), slot])
    for dy in (-1, 1):
        rowmap = rowmaps[int(dy > 0)]
        for dz, at, n in ((0, 0, rowmap.n_own), (1, rowmap.n_own, rowmap.n_hi),
                          (-1, rowmap.n_own + rowmap.n_hi, rowmap.n_lo)):
            message(steps_of(0, dy, dz), YS.at[int(dy > 0), pl.ds(at, n)],
                    YR.at[int(dy < 0), pl.ds(at, n)])
    for dx in (-1, 1):
        side = int(dx < 0)
        message(steps_of(dx, 0, 0), XS.at[pl.ds(0, 3)], XR.at[side, pl.ds(0, 3)])
        message(steps_of(dx, 0, 1), XS.at[3], XR.at[side, 3])
        message(steps_of(dx, 0, -1), XS.at[4], XR.at[side, 4])
    for dz in (1, -1):
        side = int(dz > 0)
        message(steps_of(0, 0, dz), ZS.at[side], ZR.at[side])

    relayed = []
    for at, (steps, dst, copy) in enumerate(sent):
        if upward(steps):
            onward = {a: d for a, d in steps.items() if a != "gx"}
            ok = jnp.logical_and(jnp.logical_and(exists(onward), has["gx", -1]), across)
            relayed.append((ok, pltpu.make_async_remote_copy(
                src_ref=XQ, dst_ref=dst, send_sem=send_sem.at[at], recv_sem=recv_sem.at[at],
                device_id=device(onward), device_id_type=MESH)))
    passing = pltpu.make_async_remote_copy(
        src_ref=XS.at[5], dst_ref=XQ, send_sem=send_sem.at[len(sent)],
        recv_sem=recv_sem.at[len(sent)], device_id=device({"gx": 1}), device_id_type=MESH)
    passes = jnp.logical_and(across, has["gx", 1])
    passed = jnp.logical_and(across, has["gx", -1])

    def goes(steps):
        return near_by(steps) if upward(steps) else exists(steps)

    def start(which, when=None):
        for steps, dst, copy in sent:
            if which(steps):
                ok = goes(steps)

                @pl.when(ok if when is None else jnp.logical_and(ok, when))
                def _():
                    copy.start()

    for steps, dst, copy in sent:
        @pl.when(jnp.logical_not(exists({a: -d for a, d in steps.items()})))
        def _():
            dst[...] = jnp.zeros(dst.shape, f32)

    def with_corners(steps):
        return "gy" in steps and "gx" in steps and not upward(steps)

    def with_rows(steps):
        return "gy" in steps and "gx" not in steps

    def with_columns(steps):
        return "gx" in steps and "gy" not in steps

    def with_sections(steps):
        return "gx" not in steps and "gy" not in steps

    def meet():
        pl.semaphore_wait(barrier, sum(
            exists(p).astype(jnp.int32) for p in peers if not upward(p)))

    def answer():
        for p in peers:
            if downward(p):
                @pl.when(near_by(p))
                def _():
                    pl.semaphore_signal(ready, inc=1, device_id=device(p), device_id_type=MESH)

    first_tile = jnp.logical_not(jnp.logical_or(has["gx", -1], has["gy", -1]))
    later_tile = jnp.logical_or(has["gx", -1], has["gy", -1])

    zero = jnp.zeros((8, LANES), f32)

    def clear(ref, at, n):
        ref[at:at + n] = jnp.zeros((n, LANES), f32)

    clear(Z, 0, 2)

    @pl.loop(1, nt * ext[0])
    def _(i):
        Z[pl.ds(i * ZP - 1, 3)] = jnp.zeros((3, LANES), f32)
    clear(Z, nt * ext[0] * ZP - 1, 1)
    for s in range(ext[1]):
        clear(A2Z.at[0], s * P2, 1)
        clear(A2Z.at[1], s * P2, 1)
    for s in range(ext[2]):
        clear(A3Z.at[0], s * P3, 1)
        clear(A3Z.at[1], s * P3, 1)
    EA1[...] = jnp.zeros(EA1.shape, f32)
    EA2[...] = jnp.zeros(EA2.shape, f32)
    YG[...] = jnp.zeros(YG.shape, f32)

    row8 = lax.broadcasted_iota(jnp.int32, (8, LANES), 0)
    lane = lax.broadcasted_iota(jnp.int32, (8, LANES), 1)
    nx = nt * LANES
    full, no_lo, no_hi = chain(nx, True, True), chain(nx, False, True), chain(nx, True, False)

    def spots(entries):
        x = jnp.zeros((8, LANES), f32)
        for r, c, val in entries:
            x = jnp.where(jnp.logical_and(row8 == r, lane == c), float(val), x)
        return x

    def fixes(lev, other):
        found = {}
        for c in range(nx >> (lev + 1)):
            for k, val in full[lev][c].items():
                gone = val - other[lev].get(c, {}).get(k, 0)
                if gone:
                    found[k, c] = gone
        return found

    for lev, W in ((0, W1), (1, W2), (2, W3)):
        step = 2 << lev
        mid = (nx >> (lev + 1)) // 2
        tap = {k - step * mid: w for k, w in full[lev][mid].items()}
        reach = max(tap)
        scale = 2.0 ** (-12 * (lev + 1))
        signed = jnp.where(lane < LANES // 2, lane, lane - LANES)
        delta = row8 - step * signed
        dist = jnp.abs(delta)
        base = jnp.zeros((8, LANES), f32)
        for d in range(reach + 1):
            base = jnp.where(dist == d, tap[d] * scale, base)
        lo_fix, hi_fix = fixes(lev, no_lo), fixes(lev, no_hi)
        for b, lts in blocks_of(lev, nt):
            for part in range(WIDE[lev] // LANES):
                c0 = WIDE[lev] * b + LANES * part
                for kk in range(0, len(lts) * LANES, 16):
                    pieces = []
                    for k8 in (kk, kk + 8):
                        k = lts[0] * LANES + k8
                        first = -((-(k - reach)) // step) - c0
                        last = (k + 7 + reach) // step - c0
                        if last < 0 or first >= LANES:
                            pieces.append(zero)
                            continue
                        x = pltpu.roll(base, (k // step - c0) % LANES, 1)
                        if first < 0:
                            x = jnp.where(lane <= last, x, 0.0)
                        elif last >= LANES:
                            x = jnp.where(lane >= first, x, 0.0)
                        for fix, fl in ((lo_fix, fx_lo), (hi_fix, fx_hi)):
                            here = [(r - k, c - c0, val * scale) for (r, c), val in fix.items()
                                    if k <= r < k + 8 and c0 <= c < c0 + LANES]
                            if here:
                                x = x - (1.0 - fl) * spots(here)
                        pieces.append(x)
                    w = jnp.concatenate(pieces, axis=0)
                    hi = w.astype(bf16)
                    cols = slice(part * LANES, (part + 1) * LANES)
                    if lev < 2:
                        W[b, kk:kk + 16, cols] = hi
                    else:
                        W[b, kk:kk + 16, 0:LANES] = hi
                        W[b, kk:kk + 16, LANES:2 * LANES] = (w - hi.astype(f32)).astype(bf16)

    for lev in range(3):
        n = nx >> (lev + 1)
        scale = 2.0 ** (-12 * (lev + 1))
        entries = []
        for r, c in [(0, n), (7, -1)] + ([(1, n + 1)] if HI[lev] == 2 else []):
            for k, val in full[lev][c].items():
                entries.append((r, k if k < LANES // 2 else k - nx + LANES, val * scale))
        x = spots(entries)
        hi, lo = split2(x)
        both = jnp.concatenate([hi.astype(f32), lo.astype(f32)], axis=0)
        WG[16 * lev:16 * lev + 16] = both.astype(bf16)

    def z_block(lt, r, base):
        cols = pl.ds(aligned(lt, LANES), LANES)
        x = [v[i, r:r + 8, cols] for i in range(nz)]
        for s in range(ext[0]):
            o = s - 1
            y = partial_conv(lambda i: x[i], o, 0, nz)
            if o < 0:
                y = y * fz_lo
            elif o >= m[0]:
                y = y * fz_hi
            Z[pl.ds(base + s * ZP + r + 2, 8)] = y

    def zrow(n, mz):
        row = lax.broadcasted_iota(jnp.int32, (n, LANES), 0)
        return jnp.where(row == 0, fz_lo, jnp.where(row > mz, fz_hi, 1.0))

    def edge(lt, base, slot):
        ea1, ea2, yg = EA1.at[slot], EA2.at[slot], YG.at[slot]
        src = {}

        def zy(y):
            if y not in src:
                src[y] = Z[pl.ds(base + y + 2, ext[0], ZP)]
            return src[y]
        f2, f3 = zrow(ext[1], m[1]), zrow(ext[2], m[2])
        n1, n2, n3 = rw
        rows1 = [-1, 0, 1, 2] + list(range(n1 - 6, n1 + 1))
        a2z = {}
        for k, e in enumerate(rows1):
            x = partial_conv(zy, e, 0, ny)
            ea1[k * E1P + 3:k * E1P + 3 + ext[0]] = x
            if e == -1:
                yg[0:ext[0]] = x
            elif e == n1:
                yg[16:16 + ext[0]] = x
        for k, e in enumerate(rows1):
            a2z[e] = conv(lambda j: ea1[pl.ds(k * E1P + 2 + j, ext[1], 2)]) * f2
        at = aligned(lt, 16)
        EG2[pl.ds(at, ext[1])] = a2z[-1]
        EG2[pl.ds(at + 8, ext[1])] = a2z[n1]
        rows2 = [-1, 0, n2 - 2, n2 - 1, n2, n2 + 1]
        a3z = {}
        for k, e in enumerate(rows2):
            x = partial_conv(lambda i: a2z[i], e, -1, n1 + 1)
            ea2[k * E2P + 3:k * E2P + 3 + ext[1]] = x
            if e in (-1, n2, n2 + 1):
                r = 32 + 8 * (0, n2, n2 + 1).index(max(e, 0))
                yg[r:r + ext[1]] = x
        for k, e in enumerate(rows2):
            a3z[e] = conv(lambda j: ea2[pl.ds(k * E2P + 2 + j, ext[2], 2)]) * f3
        EG3[pl.ds(at, ext[2])] = a3z[-1]
        EG3[pl.ds(at + 8, ext[2])] = a3z[n2]
        for k, e in enumerate((-1, n3, n3 + 1)):
            x = partial_conv(lambda i: a3z[i], e, -1, n2 + 2)
            yg[64 + 8 * k:64 + 8 * k + ext[2]] = x
        cols = pl.ds(aligned(lt, LANES), LANES)
        for lev in range(3):
            hi, mid = split2(yg[32 * lev:32 * lev + 32])
            YX[64 * lev:64 * lev + 32, cols] = hi
            YX[64 * lev + 32:64 * lev + 64, cols] = mid

    order3 = list(range(1, ext[2])) + [0]

    def main(lt, base, slot):
        a2, a3 = A2Z.at[slot], A3Z.at[slot]
        cols = pl.ds(aligned(lt, LANES), LANES)
        at = aligned(lt, 16)
        a2[pl.ds(1, ext[1], P2)] = EG2[pl.ds(at, ext[1])] * fy_lo
        a2[pl.ds(rw[0] + 2, ext[1], P2)] = EG2[pl.ds(at + 8, ext[1])] * fy_hi
        a3[pl.ds(1, ext[2], P3)] = EG3[pl.ds(at, ext[2])] * fy_lo
        a3[pl.ds(rw[1] + 2, ext[2], P3)] = EG3[pl.ds(at + 8, ext[2])] * fy_hi

        def reduce_sections(x, lev):
            for s in range(ext[lev]):
                y = partial_conv(lambda i: x[i + 1], s - 1, -1, len(x) - 1)
                if s == 0:
                    y = y * fz_lo
                elif s > m[lev]:
                    y = y * fz_hi
                yield s, y

        for q in range(0, rw[0], 16):
            x = []
            for s in range(ext[0]):
                half = [conv(lambda j: Z[pl.ds(base + s * ZP + 2 * (q + h) + 2 + j, 8, 2)])
                        for h in (0, 8)]
                y = jnp.concatenate(half, axis=0)
                hi, mid = split2(y)
                r = s * rw[0] + q
                LX1[r:r + 16, cols] = hi
                LX1[ext[0] * rw[0] + r:ext[0] * rw[0] + r + 16, cols] = mid
                x.append(y)
            for s, y in reduce_sections(x, 1):
                a2[s * P2 + q + 2:s * P2 + q + 18] = y
        for q in range(0, rw[1], 16):
            x = []
            for s in range(ext[1]):
                half = [conv(lambda j: a2[pl.ds(s * P2 + 2 * (q + h) + 2 + j, 8, 2)])
                        for h in (0, 8)]
                y = jnp.concatenate(half, axis=0)
                hi, mid = split2(y)
                r = s * rw[1] + q
                LX2[r:r + 16, cols] = hi
                LX2[ext[1] * rw[1] + r:ext[1] * rw[1] + r + 16, cols] = mid
                x.append(y)
            for s, y in reduce_sections(x, 2):
                a3[s * P3 + q + 2:s * P3 + q + 18] = y
        x = {}
        for s in range(ext[2]):
            x[s] = conv(lambda j: a3[pl.ds(s * P3 + 2 + j, 8, 2)])
        n = LX3.shape[0] // 2
        for i in range(0, n // 8, 2):
            pair = [x[order3[k]] if k < ext[2] else zero for k in (i, i + 1)]
            hi, mid = split2(jnp.concatenate(pair, axis=0))
            LX3[8 * i:8 * i + 16, cols] = hi
            LX3[n + 8 * i:n + 8 * i + 16, cols] = mid

    def columns(lev, rows_of):
        W = (W1, W2, W3)[lev]
        for b, lts in blocks_of(lev, nt):
            x = rows_of(slice(lts[0] * LANES, (lts[-1] + 1) * LANES))
            d = jnp.dot(x, W[b, 0:len(lts) * LANES], preferred_element_type=f32)
            n = x.shape[0] // 2
            d = d[0:n] + d[n:2 * n]
            if lev == 2:
                yield b, d[:, 0:LANES] + d[:, LANES:2 * LANES]
            else:
                for part in range(WIDE[lev] // LANES):
                    yield (b * (WIDE[lev] // LANES) + part,
                           d[:, part * LANES:(part + 1) * LANES])

    lane_k = lax.broadcasted_iota(jnp.int32, (16, LANES), 1) < LANES // 2

    def ends(ref, r, n):
        pieces = []
        for i in range(r, r + n, 16):
            a = ref[i:i + 16, 0:LANES].astype(f32)
            c = ref[i:i + 16, (nt - 1) * LANES:nt * LANES].astype(f32)
            pieces.append(jnp.where(lane_k, a, c).astype(bf16))
        return pieces

    def spill_columns(parts):
        his, mids = [], []
        for tile in parts:
            used = 0
            for lev, ref, r, n, off in tile:
                his += ends(ref, r, n)
                mids += ends(ref, r + off, n)
                used += n
            if used < LANES:
                fill = jnp.zeros((LANES - used, LANES), bf16)
                his.append(fill)
                mids.append(fill)
        rhs = jnp.concatenate(
            [jnp.concatenate(his, axis=0), jnp.concatenate(mids, axis=0)], axis=1)
        w = WG[...]
        lhs = jnp.concatenate([w, w], axis=1)
        d = lax.dot_general(lhs, rhs, (((1,), (1,)), ((), ())), preferred_element_type=f32)
        for i, tile in enumerate(parts):
            out, start = None, 0
            for lev, ref, r, n, off in tile:
                cols = slice(i * LANES, (i + 1) * LANES)
                x = d[16 * lev:16 * lev + 8, cols] + d[16 * lev + 8:16 * lev + 16, cols]
                out = x if out is None else jnp.where(lane >= start, x, out)
                start += n
            yield out

    def tile_edge(lt, slot):
        base = lt * (ext[0] * ZP)
        for r in [0] + list(range(high, ny, 8)):
            z_block(lt, r, base)
        edge(lt, base, slot)

    for c in loads[0:4]:
        c.wait()
    tile_edge(0, 0)
    tile_edge(nt - 1, 1)
    XS[5] = next(spill_columns([[(lev, YX, 64 * lev, 32, 32) for lev in range(3)]]))
    for c in loads[4:6]:
        c.wait()

    @pl.loop(0, (nt - 2) // 2)
    def _(i):
        tile_edge(1 + 2 * i, 0)
        tile_edge(2 + 2 * i, 1)

    def first_sends():
        meet()
        start(with_corners)

        @pl.when(passes)
        def _():
            passing.start()
        answer()

    @pl.when(later_tile)
    def _():
        first_sends()

    def tile_main(lt, slot):
        base = lt * (ext[0] * ZP)
        for r in range(low, high, 8):
            z_block(lt, r, base)
        main(lt, base, slot)

    for c in loads[6:8]:
        c.wait()
    tile_main(0, 0)
    tile_main(nt - 1, 1)

    for lev in range(3):
        for t, d in columns(lev, lambda cols: YX[64 * lev:64 * lev + 64, cols]):
            DS[32 * t:32 * t + 32] = d
            e, mm, h = 16 if lev == 0 else 8, m[lev], HI[lev]
            for side in (0, 1):
                rowmap = rowmaps[side]
                for k in range(h if side else 1):
                    r = 32 * t + e * (side + k)
                    slot = k * tiles[lev] + t
                    to = rowmap.own[lev] + slot * mm
                    YS[side, to:to + mm] = DS[r + 1:r + 1 + mm]
                    to = rowmap.hi[lev] + slot * h
                    YS[side, to:to + h] = DS[r + 1 + mm:r + 1 + mm + h]
                    to = rowmap.lo[lev] + slot
                    YS[side, to:to + 1] = DS[r:r + 1]

    @pl.when(later_tile)
    def _():
        start(with_rows)

    o1, o2 = ext[0] * rw[0], ext[1] * rw[1]
    o3 = LX3.shape[0] // 2
    own = [(0, LX1, rw[0] * (1 + i), LANES, o1) for i in range(0, m[0], LANES // rw[0])]
    parts = [[p] for p in own]
    parts.append([(1, LX2, rw[1], m[1] * rw[1], o2), (2, LX3, 0, m[2] * rw[2], o3)])
    parts.append([(0, LX1, rw[0] * (1 + m[0]), rw[0], o1),
                  (1, LX2, rw[1] * (1 + m[1]), 2 * rw[1], o2), (2, LX3, 16, 16, o3)])
    parts.append([(0, LX1, 0, rw[0], o1), (1, LX2, 0, rw[1], o2), (2, LX3, 32, 16, o3)])
    for i, x in enumerate(spill_columns(parts)):
        XS[i] = x
    start(with_columns, later_tile)

    loads[8].wait()

    @pl.loop(0, (nt - 2) // 2)
    def _(i):
        tile_main(1 + 2 * i, 0)
        tile_main(2 + 2 * i, 1)

    @pl.when(first_tile)
    def _():
        first_sends()
        start(with_rows)
        start(with_columns)

    @pl.when(passed)
    def _():
        passing.wait_recv()
    for ok, copy in relayed:
        @pl.when(ok)
        def _():
            copy.start()
    answers = sum(near_by(p).astype(jnp.int32) for p in peers if upward(p))

    @pl.when(answers > 0)
    def _():
        pl.semaphore_wait(ready, answers)
    start(upward)

    zat = [[0, 0, 0], [0, 0, 0]]
    at = [0, 0]
    for lev in range(3):
        for side in (0, 1):
            zat[side][lev] = at[side]
            at[side] += (HI[lev] if side else 1) * tiles[lev] * rw[lev]
    for lev, LX in ((0, LX1), (1, LX2), (2, LX3)):
        n, r = rw[lev], tiles[lev]
        for t, d in columns(lev, lambda cols: LX[:, cols]):
            for s in range(ext[lev]):
                i = order3.index(s) if lev == 2 else s
                x = d[i * n:(i + 1) * n]
                if s == 0:
                    to = zat[0][lev] + t * n
                    ZS[0, to:to + n] = x
                elif s > m[lev]:
                    to = zat[1][lev] + ((s - 1 - m[lev]) * r + t) * n
                    ZS[1, to:to + n] = x
                else:
                    to = ((s - 1) * r + t) * n
                    outs[lev][to:to + n] = x
    start(with_sections)

    def wait_all(which):
        for steps, dst, copy in sent:
            if which(steps):
                @pl.when(exists({a: -d for a, d in steps.items()}))
                def _():
                    copy.wait_recv()

    wait_all(lambda s: "gx" not in s and "gy" not in s)
    for lev in range(3):
        o, n, r = outs[lev], rw[lev], tiles[lev]
        cnt = HI[lev] * r * n
        o[0:cnt] = o[0:cnt] + ZR[1, zat[1][lev]:zat[1][lev] + cnt]
        cnt, start = r * n, (m[lev] - 1) * r * n
        o[start:start + cnt] = o[start:start + cnt] + ZR[0, zat[0][lev]:zat[0][lev] + cnt]

    for steps, dst, copy in sent:
        @pl.when(goes(steps))
        def _():
            copy.wait_send()

    @pl.when(passes)
    def _():
        passing.wait_send()
    for ok, copy in relayed:
        @pl.when(ok)
        def _():
            copy.wait_send()

    wait_all(lambda s: "gx" in s or "gy" in s)
    for lev in range(3):
        o, n, r, mm = outs[lev], rw[lev], tiles[lev], m[lev]
        pitch = r * n
        for side in (0, 1):
            rowmap = rowmaps[1 - side]
            for k in range(1 if side else HI[lev]):
                y = n - 1 if side else k
                for t in range(r):
                    slot = k * r + t
                    at = rowmap.own[lev] + slot * mm
                    x = YR[side, at:at + mm]
                    h = HI[lev]
                    at = rowmap.hi[lev] + slot * h
                    up = YR[side, at:at + h]
                    at = rowmap.lo[lev] + slot
                    down = YR[side, at:at + 1]
                    here = pl.ds(t * n + y, mm, pitch)
                    o[here] = o[here] + x
                    here = pl.ds(t * n + y, h, pitch) if h > 1 else pl.ds(t * n + y, 1)
                    o[here] = o[here] + up
                    here = pl.ds((mm - 1) * pitch + t * n + y, 1)
                    o[here] = o[here] + down


    def unpack(lo, hi):
        x = jnp.concatenate([lo, jnp.zeros((LANES - 16, LANES), f32), hi], axis=0)
        return x.T

    def add_columns(lev, here, x):
        o = outs[lev]
        lanes = lax.broadcasted_iota(jnp.int32, x.shape, 1)
        a, c = jnp.where(lanes < 2, x, 0.0), jnp.where(lanes == LANES - 1, x, 0.0)
        for t, add in ((0, a), (tiles[lev] - 1, c)):
            if tiles[lev] == 1:
                if t == 0 and add is a:
                    o[here(0)] = o[here(0)] + (a + c)
                return
            o[here(t)] = o[here(t)] + add

    def section(lev, z, x):
        n = rw[lev]
        add_columns(lev, lambda t: pl.ds((z * tiles[lev] + t) * n, n), x)

    for i in range(len(own)):
        x = unpack(XR[0, i], XR[1, i])
        for j in range(LANES // rw[0]):
            section(0, i * (LANES // rw[0]) + j, x[j * rw[0]:(j + 1) * rw[0]])
    x = unpack(XR[0, 2], XR[1, 2])
    for z in range(m[1]):
        section(1, z, x[z * rw[1]:(z + 1) * rw[1]])
    at = m[1] * rw[1]
    for z in range(m[2]):
        section(2, z, x[at + z * rw[2]:at + (z + 1) * rw[2]])
    x = unpack(XR[0, 3], XR[1, 3])
    at = 0
    for lev in range(3):
        for z in range(HI[lev]):
            section(lev, z, x[at:at + rw[lev]])
            at += rw[lev]
    x = unpack(XR[0, 4], XR[1, 4])
    at = 0
    for lev in range(3):
        section(lev, m[lev] - 1, x[at:at + rw[lev]])
        at += rw[lev]

    lane96 = lane % 32
    kind_s = jnp.where(lane < 32, lane % 16, lane % 8)
    is_up = lane96 >= jnp.where(lane < 32, 16, 8)
    top = jnp.where(lane < 32, m[0], jnp.where(lane < 64, m[1], m[2]))

    def merge(side):
        total = jnp.zeros((8, LANES), f32)
        for j, up in ((0, True), (1, False)):
            for i in range(3):
                x = XR[side, 5 + 3 * j + i]
                if i == 0:
                    ok = jnp.logical_and(kind_s >= 1, kind_s <= top)
                elif i == 1:
                    ok = kind_s > top
                else:
                    ok = kind_s == 0
                ok = jnp.logical_and(ok, is_up if up else lane96 < jnp.where(lane < 32, 16, 8))
                total = jnp.where(ok, x, total)
        return total

    x = unpack(merge(0), merge(1))
    DS[0:LANES] = x
    for lev in range(3):
        n, r, mm, h = rw[lev], tiles[lev], m[lev], HI[lev]
        pitch = r * n
        e = 16 if lev == 0 else 8
        for side in (0, 1):
            for k in range(h if side else 1):
                at = 32 * lev + e * (side + k)
                y = k if side else n - 1
                add_columns(lev, lambda t: pl.ds(t * n + y, mm, pitch), DS[at + 1:at + 1 + mm])
                add_columns(
                    lev, lambda t: pl.ds(t * n + y, h, pitch) if h > 1 else pl.ds(t * n + y, 1),
                    DS[at + 1 + mm:at + 1 + mm + h])
                add_columns(lev, lambda t: pl.ds((mm - 1) * pitch + t * n + y, 1), DS[at:at + 1])


def write_out(a1, a2, a3, out1, out2, out3, sem):
    copies = []
    for src, dst in ((a1, out1), (a2, out2), (a3, out3)):
        for t in range(src.shape[1]):
            copies.append(pltpu.make_async_copy(
                src.at[:, t], dst.at[:, :, pl.ds(t * LANES, LANES)], sem.at[len(copies)]))
    for c in copies:
        c.start()
    for c in copies:
        c.wait()


def on_device(sizes, volume):
    nz, ny, nx = volume.shape
    nt = nx // LANES
    V = pltpu.VMEM
    m = [nz >> (l + 1) for l in range(3)]
    rw = [ny >> (l + 1) for l in range(3)]
    tiles = [nt >> (l + 1) for l in range(3)]
    ext = [m[l] + 1 + HI[l] for l in range(3)]
    ZP, P2, P3 = ny + 3, rw[0] + 3, rw[1] + 3
    E1P, E2P = 2 * ext[1] + 3, 2 * ext[2] + 3
    rowmap = Rows(m, tiles, True)
    n3 = -(-ext[2] * rw[2] // 16) * 16
    zrows = sum(HI[l] * tiles[l] * rw[l] for l in range(3))
    dma = pltpu.SemaphoreType.DMA
    hbm = pl.BlockSpec(memory_space=pltpu.HBM)
    vmem = pl.BlockSpec(memory_space=pltpu.VMEM)

    def flat(n):
        return V((-(-n // 8) * 8, LANES), f32)

    def two(n):
        return V((2, -(-n // 8) * 8, LANES), f32)

    def weights(lev):
        found = blocks_of(lev, nt)
        depth = max(len(lts) for b, lts in found) * LANES
        return V((len(found), depth, 256 if lev == 2 else WIDE[lev]), bf16)

    volume = pltpu.with_memory_space_constraint(volume, pltpu.HBM)
    results = pl.pallas_call(
        functools.partial(kernel, sizes, (nz, ny, nt)),
        out_shape=tuple(V((m[l] * tiles[l] * rw[l], LANES), f32) for l in range(3)),
        in_specs=[hbm],
        out_specs=(vmem, vmem, vmem),
        scratch_shapes=[
            V((nz, ny, nx), f32),
            flat(nt * ext[0] * ZP), two(ext[1] * P2), two(ext[2] * P3),
            two(11 * E1P), two(6 * E2P), flat(16 * nt), flat(16 * nt), two(96),
            V((192, nx), bf16),
            V((2 * ext[0] * rw[0], nx), bf16), V((2 * ext[1] * rw[1], nx), bf16),
            V((2 * n3, nx), bf16),
            weights(0), weights(1), weights(2), V((48, LANES), bf16),
            flat(LANES), V((2, rowmap.total, LANES), f32), V((2, rowmap.total, LANES), f32),
            V((6, 8, LANES), f32), V((2, 11, 8, LANES), f32), V((8, LANES), f32),
            V((2, zrows, LANES), f32), V((2, zrows, LANES), f32),
            dma((9,)), dma((27,)), dma((27,)), pltpu.SemaphoreType.REGULAR,
        ],
        compiler_params=pltpu.CompilerParams(
            collective_id=0, has_side_effects=True, vmem_limit_bytes=40 << 20),
        name="pyramid",
    )(volume)
    results = [x.reshape(m[l], tiles[l], rw[l], LANES) for l, x in enumerate(results)]
    return pl.pallas_call(
        write_out,
        out_shape=tuple(
            jax.ShapeDtypeStruct((nz >> l, ny >> l, nx >> l), f32) for l in (1, 2, 3)),
        in_specs=[vmem] * 3,
        out_specs=(hbm, hbm, hbm),
        scratch_shapes=[dma((sum(tiles),))],
        compiler_params=pltpu.CompilerParams(vmem_limit_bytes=4 << 20),
        name="write_out",
    )(*results)


def solution(mesh):
    sizes = {a: mesh.shape[a] for a in AXES}
    spec = P(*AXES)
    return jax.shard_map(
        functools.partial(on_device, sizes), mesh=mesh, in_specs=(spec,),
        out_specs=(spec, spec, spec), check_vma=False)
```

```python
import functools
import itertools

import jax
import jax.numpy as jnp
import numpy as np
from jax import lax
from jax.experimental import pallas as pl
from jax.experimental.pallas import tpu as pltpu
from jax.sharding import PartitionSpec as P

LANES = 128
MESH = pl.DeviceIdType.MESH
AXES = ("gz", "gy", "gx")
TAPS = {-2: 1, -1: 4, 0: 6, 1: 4, 2: 1}
HI = (1, 2, 2)
WIDE = (256, 128, 128)
f32, bf16 = jnp.float32, jnp.bfloat16


def chain(n, lo, hi):
    prev = {i: {i: 1} for i in range(n)}
    levels = []
    for lev in range(3):
        n //= 2
        cur = {}
        for o in range(-1 if lo else 0, n + (HI[lev] if hi else 0)):
            col = {}
            for j, w in TAPS.items():
                for k, v in prev.get(2 * o + j, {}).items():
                    col[k] = col.get(k, 0) + w * v
            cur[o] = col
        levels.append(cur)
        prev = cur
    return levels


def split2(x):
    hi = x.astype(bf16)
    return hi, (x - hi.astype(f32)).astype(bf16)


def blocks_of(lev, nt):
    per = WIDE[lev] * (2 << lev) // LANES
    return [(b, list(range(max(per * b - 1, 0), min(per * (b + 1) + 1, nt))))
            for b in range(nt // per)]


class Rows:
    def __init__(self, m, tiles):
        self.own, at = [], 0
        for lev in range(3):
            self.own.append(at)
            at += HI[lev] * tiles[lev] * m[lev]
        self.n_own = -(-at // 8) * 8
        self.hi, at = [], self.n_own
        for lev in range(3):
            self.hi.append(at)
            at += HI[lev] * tiles[lev] * HI[lev]
        self.n_hi = -(-(at - self.n_own) // 8) * 8
        self.lo, at = [], self.n_own + self.n_hi
        for lev in range(3):
            self.lo.append(at)
            at += HI[lev] * tiles[lev]
        self.n_lo = -(-(at - self.n_own - self.n_hi) // 8) * 8
        self.total = self.n_own + self.n_hi + self.n_lo


def aligned(i, n):
    return i * n if isinstance(i, int) else pl.multiple_of(i * n, n)


def conv(load):
    return (load(-2) + load(2)) + 4.0 * (load(-1) + load(1)) + 6.0 * load(0)


def partial_conv(load, o, lo, hi):
    have = [j for j in TAPS if lo <= 2 * o + j < hi]
    if len(have) == 5:
        return conv(lambda j: load(2 * o + j))
    total = None
    for j in have:
        term = load(2 * o + j)
        if TAPS[j] != 1:
            term = float(TAPS[j]) * term
        total = term if total is None else total + term
    return total


def kernel(sizes, dims, vol, out1, out2, out3,
           v, Z, A2Z, A3Z, EA1, EA2, EG2, EG3, YG, YX, LX1, LX2, LX3,
           W1, W2, W3, WG, DS, YS, YR, XS, XR, ZS, ZR,
           load_sem, send_sem, recv_sem):
    nz, ny, nt = dims
    m = [nz >> 1, nz >> 2, nz >> 3]
    rw = [ny >> 1, ny >> 2, ny >> 3]
    ext = [m[l] + 1 + HI[l] for l in range(3)]
    tiles = [nt >> 1, nt >> 2, nt >> 3]
    ZP, P2, P3 = ny + 3, rw[0] + 3, rw[1] + 3
    E1P, E2P = 2 * ext[1] + 3, 2 * ext[2] + 3
    rowmap = Rows(m, tiles)
    outs = (out1, out2, out3)

    idx = {a: lax.axis_index(a) for a in AXES}
    has, near = {}, {}
    for a in AXES:
        has[a, -1], has[a, 1] = idx[a] > 0, idx[a] < sizes[a] - 1
        near[a, -1] = jnp.maximum(idx[a] - 1, 0)
        near[a, 1] = jnp.minimum(idx[a] + 1, sizes[a] - 1)

    def exists(steps):
        found = None
        for a, d in steps.items():
            found = has[a, d] if found is None else jnp.logical_and(found, has[a, d])
        return found

    def device(steps):
        return {a: near[a, d] for a, d in steps.items()}

    def flag(a, d):
        return jnp.where(has[a, d], 1.0, 0.0).astype(f32)

    fz_lo, fz_hi = flag("gz", -1), flag("gz", 1)
    fy_lo, fy_hi = flag("gy", -1), flag("gy", 1)
    fx_lo, fx_hi = flag("gx", -1), flag("gx", 1)

    peers = []
    for dx, dy, dz in itertools.product((-1, 1, 0), (-1, 1, 0), (1, -1, 0)):
        p = {a: d for a, d in (("gz", dz), ("gy", dy), ("gx", dx)) if d}
        if p:
            peers.append(p)
    barrier = pltpu.get_barrier_semaphore()

    low, high = 8, ny - 16
    loads = []
    tops, rest = ((0, low), (high, 16)), ((low, high - low),)
    ends_first = ((0, 1), (nt - 1, 1), (1, nt - 2))
    for rows, spans in ((tops, ends_first), (rest, ends_first)):
        for c0, cn in spans:
            for r0, rn in rows:
                here = (slice(None), pl.ds(r0, rn), pl.ds(c0 * LANES, cn * LANES))
                c = pltpu.make_async_copy(vol.at[here], v.at[here], load_sem.at[len(loads)])
                c.start()
                loads.append(c)
    for p in peers:
        @pl.when(exists(p))
        def _():
            pl.semaphore_signal(barrier, inc=1, device_id=device(p), device_id_type=MESH)

    segments = ((0, 0, rowmap.n_own), (1, rowmap.n_own, rowmap.n_hi),
                (-1, rowmap.n_own + rowmap.n_hi, rowmap.n_lo))
    sent = []

    def message(steps, src, dst):
        at = len(sent)
        sent.append((steps, dst, pltpu.make_async_remote_copy(
            src_ref=src, dst_ref=dst, send_sem=send_sem.at[at], recv_sem=recv_sem.at[at],
            device_id=device(steps), device_id_type=MESH)))

    def steps_of(dx, dy, dz):
        return {a: d for a, d in (("gz", dz), ("gy", dy), ("gx", dx)) if d}

    for dx in (-1, 1):
        for dy in (-1, 1):
            for dz in (0, 1, -1):
                slot = 5 + 3 * (dy < 0) + (0, 1, -1).index(dz)
                message(steps_of(dx, dy, dz), XS.at[5], XR.at[int(dx < 0), slot])
    for dy in (-1, 1):
        for dz, at, n in segments:
            message(steps_of(0, dy, dz), YS.at[int(dy > 0), pl.ds(at, n)],
                    YR.at[int(dy < 0), pl.ds(at, n)])
    for dx in (-1, 1):
        side = int(dx < 0)
        message(steps_of(dx, 0, 0), XS.at[pl.ds(0, 3)], XR.at[side, pl.ds(0, 3)])
        message(steps_of(dx, 0, 1), XS.at[3], XR.at[side, 3])
        message(steps_of(dx, 0, -1), XS.at[4], XR.at[side, 4])
    for dz in (1, -1):
        side = int(dz > 0)
        message(steps_of(0, 0, dz), ZS.at[side], ZR.at[side])

    def start(which, when=None):
        for steps, dst, copy in sent:
            if which(steps):
                ok = exists(steps)

                @pl.when(ok if when is None else jnp.logical_and(ok, when))
                def _():
                    copy.start()

    for steps, dst, copy in sent:
        @pl.when(jnp.logical_not(exists({a: -d for a, d in steps.items()})))
        def _():
            dst[...] = jnp.zeros(dst.shape, f32)

    def with_corners(steps):
        return "gy" in steps and "gx" in steps

    def with_rows(steps):
        return "gy" in steps and "gx" not in steps

    def with_columns(steps):
        return "gx" in steps and "gy" not in steps

    def with_sections(steps):
        return "gx" not in steps and "gy" not in steps

    def meet():
        pl.semaphore_wait(barrier, sum(exists(p).astype(jnp.int32) for p in peers))

    first_tile = jnp.logical_not(jnp.logical_or(has["gx", -1], has["gy", -1]))
    later_tile = jnp.logical_or(has["gx", -1], has["gy", -1])

    zero = jnp.zeros((8, LANES), f32)

    def clear(ref, at, n):
        ref[at:at + n] = jnp.zeros((n, LANES), f32)

    clear(Z, 0, 2)

    @pl.loop(1, nt * ext[0])
    def _(i):
        Z[pl.ds(i * ZP - 1, 3)] = jnp.zeros((3, LANES), f32)
    clear(Z, nt * ext[0] * ZP - 1, 1)
    for s in range(ext[1]):
        clear(A2Z.at[0], s * P2, 1)
        clear(A2Z.at[1], s * P2, 1)
    for s in range(ext[2]):
        clear(A3Z.at[0], s * P3, 1)
        clear(A3Z.at[1], s * P3, 1)
    EA1[...] = jnp.zeros(EA1.shape, f32)
    EA2[...] = jnp.zeros(EA2.shape, f32)
    YG[...] = jnp.zeros(YG.shape, f32)

    row8 = lax.broadcasted_iota(jnp.int32, (8, LANES), 0)
    lane = lax.broadcasted_iota(jnp.int32, (8, LANES), 1)
    nx = nt * LANES
    full, no_lo, no_hi = chain(nx, True, True), chain(nx, False, True), chain(nx, True, False)

    def spots(entries):
        x = jnp.zeros((8, LANES), f32)
        for r, c, val in entries:
            x = jnp.where(jnp.logical_and(row8 == r, lane == c), float(val), x)
        return x

    def fixes(lev, other):
        found = {}
        for c in range(nx >> (lev + 1)):
            for k, val in full[lev][c].items():
                gone = val - other[lev].get(c, {}).get(k, 0)
                if gone:
                    found[k, c] = gone
        return found

    for lev, W in ((0, W1), (1, W2), (2, W3)):
        step = 2 << lev
        mid = (nx >> (lev + 1)) // 2
        tap = {k - step * mid: w for k, w in full[lev][mid].items()}
        reach = max(tap)
        scale = 2.0 ** (-12 * (lev + 1))
        signed = jnp.where(lane < LANES // 2, lane, lane - LANES)
        delta = row8 - step * signed
        dist = jnp.abs(delta)
        base = jnp.zeros((8, LANES), f32)
        for d in range(reach + 1):
            base = jnp.where(dist == d, tap[d] * scale, base)
        lo_fix, hi_fix = fixes(lev, no_lo), fixes(lev, no_hi)
        for b, lts in blocks_of(lev, nt):
            for part in range(WIDE[lev] // LANES):
                c0 = WIDE[lev] * b + LANES * part
                for kk in range(0, len(lts) * LANES, 16):
                    pieces = []
                    for k8 in (kk, kk + 8):
                        k = lts[0] * LANES + k8
                        first = -((-(k - reach)) // step) - c0
                        last = (k + 7 + reach) // step - c0
                        if last < 0 or first >= LANES:
                            pieces.append(zero)
                            continue
                        x = pltpu.roll(base, (k // step - c0) % LANES, 1)
                        if first < 0:
                            x = jnp.where(lane <= last, x, 0.0)
                        elif last >= LANES:
                            x = jnp.where(lane >= first, x, 0.0)
                        for fix, fl in ((lo_fix, fx_lo), (hi_fix, fx_hi)):
                            here = [(r - k, c - c0, val * scale) for (r, c), val in fix.items()
                                    if k <= r < k + 8 and c0 <= c < c0 + LANES]
                            if here:
                                x = x - (1.0 - fl) * spots(here)
                        pieces.append(x)
                    w = jnp.concatenate(pieces, axis=0)
                    hi = w.astype(bf16)
                    cols = slice(part * LANES, (part + 1) * LANES)
                    if lev < 2:
                        W[b, kk:kk + 16, cols] = hi
                    else:
                        W[b, kk:kk + 16, 0:LANES] = hi
                        W[b, kk:kk + 16, LANES:2 * LANES] = (w - hi.astype(f32)).astype(bf16)

    for lev in range(3):
        n = nx >> (lev + 1)
        scale = 2.0 ** (-12 * (lev + 1))
        entries = []
        for r, c in [(0, n), (7, -1)] + ([(1, n + 1)] if HI[lev] == 2 else []):
            for k, val in full[lev][c].items():
                entries.append((r, k if k < LANES // 2 else k - nx + LANES, val * scale))
        x = spots(entries)
        hi, lo = split2(x)
        both = jnp.concatenate([hi.astype(f32), lo.astype(f32)], axis=0)
        WG[16 * lev:16 * lev + 16] = both.astype(bf16)

    def z_block(lt, r, base):
        cols = pl.ds(aligned(lt, LANES), LANES)
        x = [v[i, r:r + 8, cols] for i in range(nz)]
        for s in range(ext[0]):
            o = s - 1
            y = partial_conv(lambda i: x[i], o, 0, nz)
            if o < 0:
                y = y * fz_lo
            elif o >= m[0]:
                y = y * fz_hi
            Z[pl.ds(base + s * ZP + r + 2, 8)] = y

    def zrow(n, mz):
        row = lax.broadcasted_iota(jnp.int32, (n, LANES), 0)
        return jnp.where(row == 0, fz_lo, jnp.where(row > mz, fz_hi, 1.0))

    def edge(lt, base, slot):
        ea1, ea2, yg = EA1.at[slot], EA2.at[slot], YG.at[slot]
        src = {}

        def zy(y):
            if y not in src:
                src[y] = Z[pl.ds(base + y + 2, ext[0], ZP)]
            return src[y]
        f2, f3 = zrow(ext[1], m[1]), zrow(ext[2], m[2])
        n1, n2, n3 = rw
        rows1 = [-1, 0, 1, 2] + list(range(n1 - 6, n1 + 1))
        a2z = {}
        for k, e in enumerate(rows1):
            x = partial_conv(zy, e, 0, ny)
            ea1[k * E1P + 3:k * E1P + 3 + ext[0]] = x
            if e == -1:
                yg[0:ext[0]] = x
            elif e == n1:
                yg[16:16 + ext[0]] = x
        for k, e in enumerate(rows1):
            a2z[e] = conv(lambda j: ea1[pl.ds(k * E1P + 2 + j, ext[1], 2)]) * f2
        at = aligned(lt, 16)
        EG2[pl.ds(at, ext[1])] = a2z[-1]
        EG2[pl.ds(at + 8, ext[1])] = a2z[n1]
        rows2 = [-1, 0, n2 - 2, n2 - 1, n2, n2 + 1]
        a3z = {}
        for k, e in enumerate(rows2):
            x = partial_conv(lambda i: a2z[i], e, -1, n1 + 1)
            ea2[k * E2P + 3:k * E2P + 3 + ext[1]] = x
            if e in (-1, n2, n2 + 1):
                r = 32 + 8 * (0, n2, n2 + 1).index(max(e, 0))
                yg[r:r + ext[1]] = x
        for k, e in enumerate(rows2):
            a3z[e] = conv(lambda j: ea2[pl.ds(k * E2P + 2 + j, ext[2], 2)]) * f3
        EG3[pl.ds(at, ext[2])] = a3z[-1]
        EG3[pl.ds(at + 8, ext[2])] = a3z[n2]
        for k, e in enumerate((-1, n3, n3 + 1)):
            x = partial_conv(lambda i: a3z[i], e, -1, n2 + 2)
            yg[64 + 8 * k:64 + 8 * k + ext[2]] = x
        cols = pl.ds(aligned(lt, LANES), LANES)
        for lev in range(3):
            hi, mid = split2(yg[32 * lev:32 * lev + 32])
            YX[64 * lev:64 * lev + 32, cols] = hi
            YX[64 * lev + 32:64 * lev + 64, cols] = mid

    order3 = list(range(1, ext[2])) + [0]

    def main(lt, base, slot):
        a2, a3 = A2Z.at[slot], A3Z.at[slot]
        cols = pl.ds(aligned(lt, LANES), LANES)
        at = aligned(lt, 16)
        a2[pl.ds(1, ext[1], P2)] = EG2[pl.ds(at, ext[1])] * fy_lo
        a2[pl.ds(rw[0] + 2, ext[1], P2)] = EG2[pl.ds(at + 8, ext[1])] * fy_hi
        a3[pl.ds(1, ext[2], P3)] = EG3[pl.ds(at, ext[2])] * fy_lo
        a3[pl.ds(rw[1] + 2, ext[2], P3)] = EG3[pl.ds(at + 8, ext[2])] * fy_hi

        def reduce_sections(x, lev):
            for s in range(ext[lev]):
                y = partial_conv(lambda i: x[i + 1], s - 1, -1, len(x) - 1)
                if s == 0:
                    y = y * fz_lo
                elif s > m[lev]:
                    y = y * fz_hi
                yield s, y

        for q in range(0, rw[0], 16):
            x = []
            for s in range(ext[0]):
                half = [conv(lambda j: Z[pl.ds(base + s * ZP + 2 * (q + h) + 2 + j, 8, 2)])
                        for h in (0, 8)]
                y = jnp.concatenate(half, axis=0)
                hi, mid = split2(y)
                r = s * rw[0] + q
                LX1[r:r + 16, cols] = hi
                LX1[ext[0] * rw[0] + r:ext[0] * rw[0] + r + 16, cols] = mid
                x.append(y)
            for s, y in reduce_sections(x, 1):
                a2[s * P2 + q + 2:s * P2 + q + 18] = y
        for q in range(0, rw[1], 16):
            x = []
            for s in range(ext[1]):
                half = [conv(lambda j: a2[pl.ds(s * P2 + 2 * (q + h) + 2 + j, 8, 2)])
                        for h in (0, 8)]
                y = jnp.concatenate(half, axis=0)
                hi, mid = split2(y)
                r = s * rw[1] + q
                LX2[r:r + 16, cols] = hi
                LX2[ext[1] * rw[1] + r:ext[1] * rw[1] + r + 16, cols] = mid
                x.append(y)
            for s, y in reduce_sections(x, 2):
                a3[s * P3 + q + 2:s * P3 + q + 18] = y
        x = {}
        for s in range(ext[2]):
            x[s] = conv(lambda j: a3[pl.ds(s * P3 + 2 + j, 8, 2)])
        n = LX3.shape[0] // 2
        for i in range(0, n // 8, 2):
            pair = [x[order3[k]] if k < ext[2] else zero for k in (i, i + 1)]
            hi, mid = split2(jnp.concatenate(pair, axis=0))
            LX3[8 * i:8 * i + 16, cols] = hi
            LX3[n + 8 * i:n + 8 * i + 16, cols] = mid

    def columns(lev, rows_of):
        W = (W1, W2, W3)[lev]
        for b, lts in blocks_of(lev, nt):
            x = rows_of(slice(lts[0] * LANES, (lts[-1] + 1) * LANES))
            d = jnp.dot(x, W[b, 0:len(lts) * LANES], preferred_element_type=f32)
            n = x.shape[0] // 2
            d = d[0:n] + d[n:2 * n]
            if lev == 2:
                yield b, d[:, 0:LANES] + d[:, LANES:2 * LANES]
            else:
                for part in range(WIDE[lev] // LANES):
                    yield (b * (WIDE[lev] // LANES) + part,
                           d[:, part * LANES:(part + 1) * LANES])

    lane_k = lax.broadcasted_iota(jnp.int32, (16, LANES), 1) < LANES // 2

    def ends(ref, r, n):
        pieces = []
        for i in range(r, r + n, 16):
            a = ref[i:i + 16, 0:LANES].astype(f32)
            c = ref[i:i + 16, (nt - 1) * LANES:nt * LANES].astype(f32)
            pieces.append(jnp.where(lane_k, a, c).astype(bf16))
        return pieces

    def spill_columns(parts):
        his, mids = [], []
        for tile in parts:
            used = 0
            for lev, ref, r, n, off in tile:
                his += ends(ref, r, n)
                mids += ends(ref, r + off, n)
                used += n
            if used < LANES:
                fill = jnp.zeros((LANES - used, LANES), bf16)
                his.append(fill)
                mids.append(fill)
        rhs = jnp.concatenate(
            [jnp.concatenate(his, axis=0), jnp.concatenate(mids, axis=0)], axis=1)
        w = WG[...]
        lhs = jnp.concatenate([w, w], axis=1)
        d = lax.dot_general(lhs, rhs, (((1,), (1,)), ((), ())), preferred_element_type=f32)
        for i, tile in enumerate(parts):
            out, start = None, 0
            for lev, ref, r, n, off in tile:
                cols = slice(i * LANES, (i + 1) * LANES)
                x = d[16 * lev:16 * lev + 8, cols] + d[16 * lev + 8:16 * lev + 16, cols]
                out = x if out is None else jnp.where(lane >= start, x, out)
                start += n
            yield out

    def tile_edge(lt, slot):
        base = lt * (ext[0] * ZP)
        for r in [0] + list(range(high, ny, 8)):
            z_block(lt, r, base)
        edge(lt, base, slot)

    for c in loads[0:4]:
        c.wait()
    tile_edge(0, 0)
    tile_edge(nt - 1, 1)
    for c in loads[4:6]:
        c.wait()

    @pl.loop(0, (nt - 2) // 2)
    def _(i):
        tile_edge(1 + 2 * i, 0)
        tile_edge(2 + 2 * i, 1)

    def tile_main(lt, slot):
        base = lt * (ext[0] * ZP)
        for r in range(low, high, 8):
            z_block(lt, r, base)
        main(lt, base, slot)

    for lev in range(3):
        for t, d in columns(lev, lambda cols: YX[64 * lev:64 * lev + 64, cols]):
            DS[32 * t:32 * t + 32] = d
            e, mm, h = 16 if lev == 0 else 8, m[lev], HI[lev]
            for side in (0, 1):
                for k in range(h if side else 1):
                    r = 32 * t + e * (side + k)
                    slot = k * tiles[lev] + t
                    to = rowmap.own[lev] + slot * mm
                    YS[side, to:to + mm] = DS[r + 1:r + 1 + mm]
                    to = rowmap.hi[lev] + slot * h
                    YS[side, to:to + h] = DS[r + 1 + mm:r + 1 + mm + h]
                    to = rowmap.lo[lev] + slot
                    YS[side, to:to + 1] = DS[r:r + 1]
    XS[5] = next(spill_columns([[(lev, YX, 64 * lev, 32, 32) for lev in range(3)]]))

    @pl.when(later_tile)
    def _():
        meet()
        start(with_corners)
        start(with_rows)

    for c in loads[6:8]:
        c.wait()
    tile_main(0, 0)
    tile_main(nt - 1, 1)

    o1, o2 = ext[0] * rw[0], ext[1] * rw[1]
    o3 = LX3.shape[0] // 2
    own = [(0, LX1, rw[0] * (1 + i), LANES, o1) for i in range(0, m[0], LANES // rw[0])]
    parts = [[p] for p in own]
    parts.append([(1, LX2, rw[1], m[1] * rw[1], o2), (2, LX3, 0, m[2] * rw[2], o3)])
    parts.append([(0, LX1, rw[0] * (1 + m[0]), rw[0], o1),
                  (1, LX2, rw[1] * (1 + m[1]), 2 * rw[1], o2), (2, LX3, 16, 16, o3)])
    parts.append([(0, LX1, 0, rw[0], o1), (1, LX2, 0, rw[1], o2), (2, LX3, 32, 16, o3)])
    for i, x in enumerate(spill_columns(parts)):
        XS[i] = x
    start(with_columns, later_tile)

    loads[8].wait()

    @pl.loop(0, (nt - 2) // 2)
    def _(i):
        tile_main(1 + 2 * i, 0)
        tile_main(2 + 2 * i, 1)

    @pl.when(first_tile)
    def _():
        meet()
        start(with_corners)
        start(with_rows)
        start(with_columns)

    zat = [[0, 0, 0], [0, 0, 0]]
    at = [0, 0]
    for lev in range(3):
        for side in (0, 1):
            zat[side][lev] = at[side]
            at[side] += (HI[lev] if side else 1) * tiles[lev] * rw[lev]
    for lev, LX in ((0, LX1), (1, LX2), (2, LX3)):
        n, r = rw[lev], tiles[lev]
        for t, d in columns(lev, lambda cols: LX[:, cols]):
            for s in range(ext[lev]):
                i = order3.index(s) if lev == 2 else s
                x = d[i * n:(i + 1) * n]
                if s == 0:
                    to = zat[0][lev] + t * n
                    ZS[0, to:to + n] = x
                elif s > m[lev]:
                    to = zat[1][lev] + ((s - 1 - m[lev]) * r + t) * n
                    ZS[1, to:to + n] = x
                else:
                    to = ((s - 1) * r + t) * n
                    outs[lev][to:to + n] = x
    start(with_sections)

    def wait_all(which):
        for steps, dst, copy in sent:
            if which(steps):
                @pl.when(exists({a: -d for a, d in steps.items()}))
                def _():
                    copy.wait_recv()

    wait_all(lambda s: "gx" not in s and "gy" not in s)
    for lev in range(3):
        o, n, r = outs[lev], rw[lev], tiles[lev]
        cnt = HI[lev] * r * n
        o[0:cnt] = o[0:cnt] + ZR[1, zat[1][lev]:zat[1][lev] + cnt]
        cnt, start = r * n, (m[lev] - 1) * r * n
        o[start:start + cnt] = o[start:start + cnt] + ZR[0, zat[0][lev]:zat[0][lev] + cnt]

    for steps, dst, copy in sent:
        @pl.when(exists(steps))
        def _():
            copy.wait_send()

    wait_all(lambda s: "gx" in s or "gy" in s)
    for lev in range(3):
        o, n, r, mm = outs[lev], rw[lev], tiles[lev], m[lev]
        pitch = r * n
        for side in (0, 1):
            for k in range(1 if side else HI[lev]):
                y = n - 1 if side else k
                for t in range(r):
                    slot = k * r + t
                    at = rowmap.own[lev] + slot * mm
                    x = YR[side, at:at + mm]
                    h = HI[lev]
                    at = rowmap.hi[lev] + slot * h
                    up = YR[side, at:at + h]
                    at = rowmap.lo[lev] + slot
                    down = YR[side, at:at + 1]
                    here = pl.ds(t * n + y, mm, pitch)
                    o[here] = o[here] + x
                    here = pl.ds(t * n + y, h, pitch) if h > 1 else pl.ds(t * n + y, 1)
                    o[here] = o[here] + up
                    here = pl.ds((mm - 1) * pitch + t * n + y, 1)
                    o[here] = o[here] + down


    def unpack(lo, hi):
        x = jnp.concatenate([lo, jnp.zeros((LANES - 16, LANES), f32), hi], axis=0)
        return x.T

    def add_columns(lev, here, x):
        o = outs[lev]
        lanes = lax.broadcasted_iota(jnp.int32, x.shape, 1)
        a, c = jnp.where(lanes < 2, x, 0.0), jnp.where(lanes == LANES - 1, x, 0.0)
        for t, add in ((0, a), (tiles[lev] - 1, c)):
            if tiles[lev] == 1:
                if t == 0 and add is a:
                    o[here(0)] = o[here(0)] + (a + c)
                return
            o[here(t)] = o[here(t)] + add

    def section(lev, z, x):
        n = rw[lev]
        add_columns(lev, lambda t: pl.ds((z * tiles[lev] + t) * n, n), x)

    for i in range(len(own)):
        x = unpack(XR[0, i], XR[1, i])
        for j in range(LANES // rw[0]):
            section(0, i * (LANES // rw[0]) + j, x[j * rw[0]:(j + 1) * rw[0]])
    x = unpack(XR[0, 2], XR[1, 2])
    for z in range(m[1]):
        section(1, z, x[z * rw[1]:(z + 1) * rw[1]])
    at = m[1] * rw[1]
    for z in range(m[2]):
        section(2, z, x[at + z * rw[2]:at + (z + 1) * rw[2]])
    x = unpack(XR[0, 3], XR[1, 3])
    at = 0
    for lev in range(3):
        for z in range(HI[lev]):
            section(lev, z, x[at:at + rw[lev]])
            at += rw[lev]
    x = unpack(XR[0, 4], XR[1, 4])
    at = 0
    for lev in range(3):
        section(lev, m[lev] - 1, x[at:at + rw[lev]])
        at += rw[lev]

    lane96 = lane % 32
    kind_s = jnp.where(lane < 32, lane % 16, lane % 8)
    is_up = lane96 >= jnp.where(lane < 32, 16, 8)
    top = jnp.where(lane < 32, m[0], jnp.where(lane < 64, m[1], m[2]))

    def merge(side):
        total = jnp.zeros((8, LANES), f32)
        for j, up in ((0, True), (1, False)):
            for i in range(3):
                x = XR[side, 5 + 3 * j + i]
                if i == 0:
                    ok = jnp.logical_and(kind_s >= 1, kind_s <= top)
                elif i == 1:
                    ok = kind_s > top
                else:
                    ok = kind_s == 0
                ok = jnp.logical_and(ok, is_up if up else lane96 < jnp.where(lane < 32, 16, 8))
                total = jnp.where(ok, x, total)
        return total

    x = unpack(merge(0), merge(1))
    DS[0:LANES] = x
    for lev in range(3):
        n, r, mm, h = rw[lev], tiles[lev], m[lev], HI[lev]
        pitch = r * n
        e = 16 if lev == 0 else 8
        for side in (0, 1):
            for k in range(h if side else 1):
                at = 32 * lev + e * (side + k)
                y = k if side else n - 1
                add_columns(lev, lambda t: pl.ds(t * n + y, mm, pitch), DS[at + 1:at + 1 + mm])
                add_columns(
                    lev, lambda t: pl.ds(t * n + y, h, pitch) if h > 1 else pl.ds(t * n + y, 1),
                    DS[at + 1 + mm:at + 1 + mm + h])
                add_columns(lev, lambda t: pl.ds((mm - 1) * pitch + t * n + y, 1), DS[at:at + 1])


def write_out(a1, a2, a3, out1, out2, out3, sem):
    copies = []
    for src, dst in ((a1, out1), (a2, out2), (a3, out3)):
        for t in range(src.shape[1]):
            copies.append(pltpu.make_async_copy(
                src.at[:, t], dst.at[:, :, pl.ds(t * LANES, LANES)], sem.at[len(copies)]))
    for c in copies:
        c.start()
    for c in copies:
        c.wait()


def on_device(sizes, volume):
    nz, ny, nx = volume.shape
    nt = nx // LANES
    V = pltpu.VMEM
    m = [nz >> (l + 1) for l in range(3)]
    rw = [ny >> (l + 1) for l in range(3)]
    tiles = [nt >> (l + 1) for l in range(3)]
    ext = [m[l] + 1 + HI[l] for l in range(3)]
    ZP, P2, P3 = ny + 3, rw[0] + 3, rw[1] + 3
    E1P, E2P = 2 * ext[1] + 3, 2 * ext[2] + 3
    rowmap = Rows(m, tiles)
    n3 = -(-ext[2] * rw[2] // 16) * 16
    zrows = sum(HI[l] * tiles[l] * rw[l] for l in range(3))
    dma = pltpu.SemaphoreType.DMA
    hbm = pl.BlockSpec(memory_space=pltpu.HBM)
    vmem = pl.BlockSpec(memory_space=pltpu.VMEM)

    def flat(n):
        return V((-(-n // 8) * 8, LANES), f32)

    def two(n):
        return V((2, -(-n // 8) * 8, LANES), f32)

    def weights(lev):
        found = blocks_of(lev, nt)
        depth = max(len(lts) for b, lts in found) * LANES
        return V((len(found), depth, 256 if lev == 2 else WIDE[lev]), bf16)

    volume = pltpu.with_memory_space_constraint(volume, pltpu.HBM)
    results = pl.pallas_call(
        functools.partial(kernel, sizes, (nz, ny, nt)),
        out_shape=tuple(V((m[l] * tiles[l] * rw[l], LANES), f32) for l in range(3)),
        in_specs=[hbm],
        out_specs=(vmem, vmem, vmem),
        scratch_shapes=[
            V((nz, ny, nx), f32),
            flat(nt * ext[0] * ZP), two(ext[1] * P2), two(ext[2] * P3),
            two(11 * E1P), two(6 * E2P), flat(16 * nt), flat(16 * nt), two(96),
            V((192, nx), bf16),
            V((2 * ext[0] * rw[0], nx), bf16), V((2 * ext[1] * rw[1], nx), bf16),
            V((2 * n3, nx), bf16),
            weights(0), weights(1), weights(2), V((48, LANES), bf16),
            flat(LANES), V((2, rowmap.total, LANES), f32), V((2, rowmap.total, LANES), f32),
            V((6, 8, LANES), f32), V((2, 11, 8, LANES), f32),
            V((2, zrows, LANES), f32), V((2, zrows, LANES), f32),
            dma((9,)), dma((26,)), dma((26,)),
        ],
        compiler_params=pltpu.CompilerParams(
            collective_id=0, has_side_effects=True, vmem_limit_bytes=40 << 20),
        name="pyramid",
    )(volume)
    results = [x.reshape(m[l], tiles[l], rw[l], LANES) for l, x in enumerate(results)]
    return pl.pallas_call(
        write_out,
        out_shape=tuple(
            jax.ShapeDtypeStruct((nz >> l, ny >> l, nx >> l), f32) for l in (1, 2, 3)),
        in_specs=[vmem] * 3,
        out_specs=(hbm, hbm, hbm),
        scratch_shapes=[dma((sum(tiles),))],
        compiler_params=pltpu.CompilerParams(vmem_limit_bytes=4 << 20),
        name="write_out",
    )(*results)


def solution(mesh):
    sizes = {a: mesh.shape[a] for a in AXES}
    spec = P(*AXES)
    return jax.shard_map(
        functools.partial(on_device, sizes), mesh=mesh, in_specs=(spec,),
        out_specs=(spec, spec, spec), check_vma=False)
```
